256 devices in a mesh: lon: 16 (over z, y_lo), lat: 16 (over x, y_hi, core).
Axes of the slice: x: 4, y: 4 (y_hi: 2, y_lo: 2; y = y_hi * 2 + y_lo), z: 8, core: 2. Of those that a mesh axis runs over, the one named last changes fastest.
Arguments:
- velocity: bfloat16 [3, 75, 512, 4096], P(None, None, 'lat', 'lon'), may hold values from -1.5 to 1.5
- offsets: float32 [3, 16, 12288], P(None, 'lat', 'lon'), may hold values from 0 to 1
- cells: int32 [3, 16, 12288], P(None, 'lat', 'lon'), may hold values from 0 to 255, as said below
- counts: int32 [16, 16], P('lat', 'lon'), may hold values from 192 to 576, as said below
- moves: int32 [16, 12288], P('lat', 'lon'), may hold values from 0 to 4, as said below
Outputs:
- new_offsets: float32 [3, 16, 12288], P(None, 'lat', 'lon')
- new_cells: int32 [3, 16, 12288], P(None, 'lat', 'lon')
- new_counts: int32 [16, 16], P('lat', 'lon')
The draws below stay inside these ranges and needn't reach their ends.
Inputs may be any that keep to these rules, and one draw needn't show every extreme that they name: `cells`: values from 0 to 255, 31 and 73 for i, j, k. A valid slot with move 1 has i = 255, move 2 i = 0, move 3 j = 31, move 4 j = 0. `counts`: between 192 and 576; the upper bound is reached by some tile in every draw. `moves`: invalid slots have 0. In each tile at most 48 valid particles have each nonzero move, and in every draw some tile has exactly 48 for each move. Tiles of row 0 have no move 4.
All inputs are finite; a program needn't handle non-finite values.
Results may differ from the reference program's by a relative error of at most 0.00093.
Values may be sent and summed in bfloat16 or wider, within the bound.
A program may use at most 64 MiB of HBM per device.

```python
import jax
import jax.numpy as jnp
from jax import lax

KZ = 75
CX = 256
CY = 32
P_SIZE = 768
NX = 4096
NY = 512
N_LON = 16
N_LAT = 16


def particle_plan(key):
    tiles = N_LAT * N_LON
    limit = P_SIZE // 16
    live = jax.random.randint(jax.random.fold_in(key, 101), (tiles,), 4 * limit, P_SIZE - 4 * limit + 1)
    live = live.at[jax.random.randint(jax.random.fold_in(key, 102), (), 0, tiles)].set(P_SIZE - 4 * limit)
    movers = jax.random.randint(jax.random.fold_in(key, 103), (tiles, 4), 0, limit + 1)
    lat_of = jnp.arange(tiles, dtype=jnp.int32) // N_LON
    movers = movers.at[:, 3].set(jnp.where(lat_of == 0, 0, movers[:, 3]))
    for code in range(3):
        chosen = jax.random.randint(jax.random.fold_in(key, 110 + code), (), 0, tiles)
        movers = movers.at[chosen, code].set(limit)
    southern = N_LON + jax.random.randint(jax.random.fold_in(key, 114), (), 0, tiles - N_LON)
    movers = movers.at[southern, 3].set(limit)
    tile_keys = jax.random.split(jax.random.fold_in(key, 104), tiles)
    order = jax.vmap(lambda single: jax.random.permutation(single, P_SIZE))(tile_keys).astype(jnp.int32)
    slot = jnp.arange(P_SIZE, dtype=jnp.int32)
    valid = slot[None, :] < live[:, None]

    def ranking(pair):
        keys, alive = pair
        return jnp.sum((alive[None, :] & (keys[None, :] < keys[:, None])).astype(jnp.int32), axis=1)
    rank = lax.map(ranking, (order, valid))
    bounds = jnp.cumsum(movers, axis=1)
    motion = jnp.where(rank < bounds[:, 0:1], 1, jnp.where(rank < bounds[:, 1:2], 2, jnp.where(rank < bounds[:, 2:3], 3, jnp.where(rank < bounds[:, 3:4], 4, 0))))
    motion = jnp.where(valid, motion, 0).astype(jnp.int32)
    col_i = jax.random.randint(jax.random.fold_in(key, 105), (tiles, P_SIZE), 0, CX)
    row_j = jax.random.randint(jax.random.fold_in(key, 106), (tiles, P_SIZE), 0, CY)
    lev_k = jax.random.randint(jax.random.fold_in(key, 107), (tiles, P_SIZE), 0, KZ - 1)
    col_i = jnp.where(motion == 1, CX - 1, jnp.where(motion == 2, 0, col_i))
    row_j = jnp.where(motion == 3, CY - 1, jnp.where(motion == 4, 0, row_j))
    cellpos = jnp.stack([col_i, row_j, lev_k]).astype(jnp.int32).reshape(3, N_LAT, N_LON * P_SIZE)
    return (live.astype(jnp.int32).reshape(N_LAT, N_LON), motion.reshape(N_LAT, N_LON * P_SIZE), cellpos)


def draw_cells(key, part):
    return particle_plan(key)[2]


def draw_counts(key, part):
    return particle_plan(key)[0]


def draw_moves(key, part):
    return particle_plan(key)[1]


def steps_of(own_key, dims, pieces, least, top_value):
    gain, own = 1.0, jax.random.fold_in(own_key, 6)
    for dim, shards_of in pieces:
        steps = jnp.exp(jax.random.uniform(jax.random.fold_in(own, dim), (shards_of,), jnp.float32, least / len(pieces), top_value / len(pieces)))
        gain = gain * jnp.repeat(steps, dims[dim] // shards_of).reshape([-1 if axis == dim else 1 for axis in range(len(dims))])
    return gain


def scatter_about(stream_key, shape, spread, most, pieces=(), kind=jnp.bfloat16):
    array = jax.random.normal(stream_key, shape, jnp.float32) * spread
    if len(pieces) > 0:
        array = steps_of(stream_key, shape, pieces, -0.22, 0.18) * array
    return jnp.clip(array, min=-most, max=most).astype(kind)


def setup_inputs(seed: int = 0) -> dict:
    streams_of = jax.random.split(jax.random.key(seed), 6)
    velocity = scatter_about(streams_of[0], (3, KZ, NY, NX), 0.3, 1.5, ((2, 16), (3, 16)))
    offsets = jnp.clip(1.0 * jax.random.uniform(streams_of[1], (3, N_LAT, N_LON * P_SIZE), jnp.float32) ** steps_of(streams_of[1], (3, N_LAT, N_LON * P_SIZE), ((1, 16), (2, 16)), -0.2, 0.2), 0.0, 1.0)
    cells = draw_cells(jax.random.fold_in(streams_of[5], 71), 0)
    counts = draw_counts(jax.random.fold_in(streams_of[5], 71), 0)
    moves = draw_moves(jax.random.fold_in(streams_of[5], 71), 0)
    return dict(velocity=velocity, offsets=offsets, cells=cells, counts=counts, moves=moves)


def fetch(velocity, level, row, column):
    inside = velocity[:, level, jnp.minimum(row, NY - 1), column % NX].astype(jnp.float32)
    mirrored = -velocity[:, level, NY - 1, (NX - column) % NX].astype(jnp.float32)
    return jnp.where(row == NY, mirrored, inside)


def rounded(value):
    half = lax.optimization_barrier(value.astype(jnp.bfloat16))
    return half.astype(jnp.float32)


def sample(velocity, position, grow, gcol, level):
    a, b, c = position[0], position[1], position[2]
    weights = [rounded((1.0 - b) * (1.0 - c)), rounded(b * (1.0 - c)), rounded((1.0 - b) * c), rounded(b * c)]
    corners = [(0, 0), (0, 1), (1, 0), (1, 1)]
    sums = []
    for shift in range(2):
        total = jnp.zeros((3,) + a.shape, jnp.float32)
        for weight, (dk, dj) in zip(weights, corners):
            total = total + weight * fetch(velocity, level + dk, grow + dj, gcol + shift)
        sums.append(total)
    return (1.0 - a) * sums[0] + a * sums[1]


def reference(velocity, offsets, cells, counts, moves):
    tiles = N_LAT * N_LON
    position = offsets.reshape(3, N_LAT, N_LON, P_SIZE)
    cellpos = cells.reshape(3, N_LAT, N_LON, P_SIZE)
    motion = moves.reshape(N_LAT, N_LON, P_SIZE)
    lat_id = jnp.arange(N_LAT, dtype=jnp.int32)[:, None, None]
    lon_id = jnp.arange(N_LON, dtype=jnp.int32)[None, :, None]
    gcol = lon_id * CX + cellpos[0]
    grow = lat_id * CY + cellpos[1]
    level = cellpos[2]
    first = sample(velocity, position, grow, gcol, level)
    middle = position + 0.5 * first
    moved = position + sample(velocity, middle, grow, gcol, level)
    na, nb, nc = moved[0], moved[1], moved[2]
    top = lat_id == N_LAT - 1
    slot = jnp.arange(P_SIZE, dtype=jnp.int32)[None, None, :]
    valid = slot < counts[:, :, None]
    fold = (motion == 3) & top
    new_a = jnp.where(motion == 1, na - 1.0, jnp.where(motion == 2, na + 1.0, jnp.where(fold, 1.0 - na, na)))
    new_b = jnp.where(motion == 3, jnp.where(top, 2.0 - nb, nb - 1.0), jnp.where(motion == 4, nb + 1.0, nb))
    new_i = jnp.where(motion == 1, 0, jnp.where(motion == 2, CX - 1, jnp.where(fold, CX - 1 - cellpos[0], cellpos[0])))
    new_j = jnp.where(motion == 3, jnp.where(top, CY - 1, 0), jnp.where(motion == 4, CY - 1, cellpos[1]))
    rank = jnp.zeros((N_LAT, N_LON, P_SIZE), jnp.int32)
    tallies = []
    for code in range(5):
        chosen = (valid & (motion == code)).astype(jnp.int32)
        rank = rank + jnp.where(motion == code, jnp.cumsum(chosen, axis=2) - chosen, 0)
        tallies.append(jnp.sum(chosen, axis=2))
    zero_row = jnp.zeros((1, N_LON), jnp.int32)
    top_rows = (jnp.arange(N_LAT, dtype=jnp.int32) == N_LAT - 1)[:, None]
    groups = jnp.stack([
        tallies[0],
        jnp.roll(tallies[1], 1, axis=1),
        jnp.roll(tallies[2], -1, axis=1),
        jnp.concatenate([zero_row, tallies[3][:-1]], axis=0),
        jnp.concatenate([tallies[4][1:], zero_row], axis=0),
        jnp.where(top_rows, tallies[3][:, ::-1], 0),
    ], axis=-1)
    bases = jnp.cumsum(groups, axis=-1) - groups
    new_counts = jnp.sum(groups, axis=-1).astype(jnp.int32)
    group = jnp.where(motion == 0, 0, jnp.where(motion == 1, 1, jnp.where(motion == 2, 2, jnp.where(motion == 4, 4, jnp.where(top, 5, 3)))))
    dest_lat = lat_id + jnp.where((motion == 3) & (~top), 1, 0) - jnp.where(motion == 4, 1, 0)
    dest_lon = (lon_id + jnp.where(motion == 1, 1, 0) - jnp.where(motion == 2, 1, 0)) % N_LON
    dest_lon = jnp.where(fold, N_LON - 1 - lon_id, dest_lon)
    dest_lat = jnp.clip(dest_lat, 0, N_LAT - 1).astype(jnp.int32)
    dest_lon = dest_lon.astype(jnp.int32)
    place = bases[dest_lat, dest_lon, group] + rank
    target = jnp.where(valid, (dest_lat * N_LON + dest_lon) * P_SIZE + place, tiles * P_SIZE).reshape(-1)
    floats = jnp.stack([new_a, new_b, nc]).reshape(3, -1)
    ints = jnp.stack([new_i, new_j, level]).astype(jnp.int32).reshape(3, -1)
    out_float = jnp.zeros((3, tiles * P_SIZE + 1), jnp.float32).at[:, target].set(floats)
    out_int = jnp.zeros((3, tiles * P_SIZE + 1), jnp.int32).at[:, target].set(ints)
    new_offsets = out_float[:, :tiles * P_SIZE].reshape(3, N_LAT, N_LON * P_SIZE)
    new_cells = out_int[:, :tiles * P_SIZE].reshape(3, N_LAT, N_LON * P_SIZE)
    return new_offsets, new_cells, new_counts
```

```python
import functools

import jax
import jax.numpy as jnp
from jax import lax
from jax.experimental import pallas as pl
from jax.experimental.pallas import tpu as pltpu
from jax.sharding import PartitionSpec as P

MESH = pl.DeviceIdType.MESH
CAP = 48
LANES = 128
F32, BF16, I32 = jnp.float32, jnp.bfloat16, jnp.int32
NT = (((1,), (1,)), ((), ()))
TN = (((0,), (0,)), ((), ()))


def iota(shape, dim):
    return lax.broadcasted_iota(I32, shape, dim)


def thirds(x):
    high = x.astype(BF16)
    rest = x - high.astype(F32)
    mid = rest.astype(BF16)
    low = (rest - mid.astype(F32)).astype(BF16)
    return jnp.concatenate([high.astype(F32), mid.astype(F32), low.astype(F32)], axis=0).astype(BF16)


def placed(records, target, size):
    onehot = jnp.where(iota((size, target.shape[1]), 0) == target, 1.0, 0.0).astype(BF16)
    out = lax.dot_general(thirds(records), onehot, NT, preferred_element_type=F32)
    return out[0:8] + out[8:16] + out[16:24]


def velocity_at(corners, a_row, b_row, c_row):
    sub = iota((8, a_row.shape[1]), 0)
    wb = jnp.where(sub < 4, 1.0 - b_row, b_row)
    w0 = (wb * (1.0 - c_row)).astype(BF16).astype(F32)
    w1 = (wb * c_row).astype(BF16).astype(F32)
    sums = []
    for d in range(2):
        s = w0 * corners[0][d] + w1 * corners[1][d]
        sums.append(s + pltpu.roll(s, 4, 0))
    return (1.0 - a_row) * sums[0] + a_row * sums[1]


def kernel(
    dims, vel_hbm, off_ref, cell_ref, cell_smem, count_smem, move_ref,
    new_off, new_cell, new_count,
    vel, table, gathered, posit, ect, nrow, nfold, cnr, cfold, ect_in, nrow_in, cnr_in,
    pack, pack_in, vsem, send, recv, lsem,
):
    depth, rows, cols, slots, live, n_lat, n_lon = dims
    wide = pl.cdiv(live, LANES) * LANES
    tiles = wide // LANES
    level = rows * 4
    span = table.shape[0] // 3
    r, p = lax.axis_index("lat"), lax.axis_index("lon")
    east, west = lax.rem(p + 1, n_lon), lax.rem(p + n_lon - 1, n_lon)
    across, corner = n_lon - 1 - p, lax.rem(n_lon - p, n_lon)
    top = r == n_lat - 1
    away = jnp.logical_and(top, corner != p)

    loads = [pltpu.make_async_copy(vel_hbm.at[c], vel.at[c], vsem.at[c]) for c in range(3)]
    for load in loads:
        load.start()

    barrier = pltpu.get_barrier_semaphore()

    def greet(lat, lon):
        pl.semaphore_signal(barrier, inc=1, device_id=(lon, lat), device_id_type=MESH)

    greet(r, east)
    greet(r, west)

    @pl.when(r < n_lat - 1)
    def _():
        greet(r + 1, p)
        greet(r + 1, east)

    @pl.when(r > 0)
    def _():
        greet(r - 1, p)

    @pl.when(top)
    def _():
        greet(r, across)

    @pl.when(away)
    def _():
        greet(r, corner)

    lane = iota((8, LANES), 1)
    lane_rows = iota((rows, LANES), 1)
    for part in range(3):
        table[pl.ds(part * span + depth * level, span - depth * level), :] = jnp.zeros(
            (span - depth * level, LANES), F32
        )
    cnr[...] = jnp.zeros_like(cnr)
    for c in range(3):
        loads[c].wait()

        def build(k, column):
            low = vel[c, k, :, 0:LANES].astype(F32)
            high = vel[c, k, :, LANES : 2 * LANES].astype(F32)
            seam = jnp.where(lane_rows == LANES - 1, low, high)
            for s in range(rows // 8):
                at = k * level + 32 * s + c
                part = slice(8 * s, 8 * s + 8)
                table[pl.ds(at, 8, stride=4), :] = low[part]
                table[pl.ds(at + span, 8, stride=4), :] = seam[part]
                table[pl.ds(at + 2 * span, 8, stride=4), :] = high[part]
            return jnp.where(lane_rows == k, pltpu.roll(low, k, 1), column)

        column = lax.fori_loop(0, depth, build, jnp.zeros((rows, LANES), F32))
        ect[c] = column.astype(BF16)
        cnr[c : c + 1, :] = column[0:1]

        @pl.when(top)
        def _(c=c, column=column):
            cfold[c : c + 1, :] = column[rows - 1 : rows]

    def edge(target, row):
        for c in range(3):
            for half in range(2):
                for block in range(nrow.shape[0] // 16):
                    at = 2 * half * span + block * 16 * level + 4 * row + c
                    pair = [table[pl.ds(at + u * 8 * level, 8, stride=level), :] for u in range(2)]
                    target[pl.ds(block * 16, 16), pl.ds(c * cols + half * LANES, LANES)] = jnp.concatenate(
                        pair, axis=0
                    ).astype(BF16)

    edge(nrow, 0)

    @pl.when(top)
    def _():
        edge(nfold, rows - 1)

    def remote(src, dst, s, t, lat, lon):
        return pltpu.make_async_remote_copy(
            src, dst, send.at[s], recv.at[t], device_id=(lon, lat), device_id_type=MESH
        )

    ect_out = remote(ect, ect_in, 0, 0, r, west)
    row_out = remote(nrow, nrow_in, 1, 1, r - 1, p)
    cnr_out = remote(cnr, cnr_in, 2, 2, r - 1, west)
    fold_out = remote(nfold, nrow_in, 3, 1, r, across)
    cfold_out = remote(cfold, cnr_in, 4, 2, r, corner)
    cfold_here = pltpu.make_async_copy(cfold, cnr_in, lsem)

    peers = 2 + 2 * (r > 0).astype(I32) + (r < n_lat - 1).astype(I32) + top.astype(I32) + away.astype(I32)
    pl.semaphore_wait(barrier, peers)

    @pl.when(r > 0)
    def _():
        row_out.start()
        cnr_out.start()

    @pl.when(top)
    def _():
        fold_out.start()

    @pl.when(away)
    def _():
        cfold_out.start()

    @pl.when(jnp.logical_and(top, corner == p))
    def _():
        cfold_here.start()

    ect_out.start()

    for block in range(tiles):
        def gather(step, accs):
            accs = list(accs)
            base = step * 8
            ahead = lane - base
            for u in range(8):
                slot = block * LANES + base + u
                i, j, k = (cell_smem[n, 0, slot] for n in range(3))
                part = jnp.where(i == LANES - 1, span, jnp.where(i >= LANES, 2 * span, 0))
                at = part + k * level + 4 * j
                shift = (base + u - i) & (LANES - 1)
                here = ahead == u
                there = (ahead == u + 1) if u < 7 else ((lane == ((base + 8) & (LANES - 1))))
                for dk in range(2):
                    turned = pltpu.roll(table[pl.ds(at + dk * level, 8), :], shift, 1)
                    accs[2 * dk] = jnp.where(here, turned, accs[2 * dk])
                    accs[2 * dk + 1] = jnp.where(there, turned, accs[2 * dk + 1])
            return tuple(accs)

        count = min(LANES, live - block * LANES)
        zero = jnp.zeros((8, LANES), F32)
        accs = lax.fori_loop(0, count // 8, gather, (zero,) * 4)
        for dk in range(2):
            gathered[dk, 0, :, pl.ds(block * LANES, LANES)] = accs[2 * dk]
            gathered[dk, 1, :, pl.ds(block * LANES, LANES)] = pltpu.roll(accs[2 * dk + 1], LANES - 1, 1)

    sub = iota((8, wide), 0)
    i_row, j_row, k_row = (cell_ref[n, :, 0:wide] for n in range(3))
    motion = move_ref[:, 0:wide]
    valid = iota((1, wide), 1) < count_smem[0, 0]
    chosen = jnp.where((sub == motion) & valid, 1.0, 0.0)
    before = jnp.where(iota((LANES, LANES), 0) < iota((LANES, LANES), 1), 1.0, 0.0).astype(BF16)
    upto = jnp.concatenate([before, jnp.ones((LANES, LANES), BF16)], axis=1)
    total = jnp.zeros((8, LANES), F32)
    ranks = []
    for t in range(tiles):
        sums = jnp.dot(
            chosen[:, t * LANES : (t + 1) * LANES].astype(BF16), upto, preferred_element_type=F32
        )
        ranks.append(sums[:, :LANES] + total)
        total = total + sums[:, LANES:]
    rank = jnp.concatenate(ranks, axis=1)
    stay_to = jnp.where(chosen[0:1] > 0.5, rank[0:1], -1.0).astype(I32)
    slot_to = rank + (LANES * (sub - 1)).astype(F32)
    leaving = (sub >= 1) & (chosen > 0.5)
    leave_to = (jnp.sum(jnp.where(leaving, slot_to + 1.0, 0.0), axis=0, keepdims=True) - 1.0).astype(I32)
    folding = (motion == 3) & top
    last_i, last_j = cols - 1, rows - 1
    new_i = jnp.where(
        motion == 1, 0, jnp.where(motion == 2, last_i, jnp.where(folding, last_i - i_row, i_row))
    )
    new_j = jnp.where(
        motion == 3, jnp.where(top, last_j, 0), jnp.where(motion == 4, last_j, j_row)
    )
    code = (1 + new_i + cols * (new_j + rows * k_row)).astype(F32)

    at_level = [
        jnp.where(iota((LANES, wide), 0) == k_row + dk, 1.0, 0.0).astype(BF16) for dk in range(2)
    ]
    first_col = jnp.where(top, cols - i_row, i_row)
    second_col = jnp.where(top, cols - 1 - i_row, i_row + 1)
    sign = jnp.where(top, -1.0, 1.0)

    ect_out.wait_recv()
    eastern = [[None, None], [None, None]]
    for dk in range(2):
        found = lax.dot_general(
            ect_in[...].reshape(3 * rows, LANES), at_level[dk], (((1,), (0,)), ((), ())),
            preferred_element_type=F32,
        )
        row_id = iota((rows, wide), 0)
        out = jnp.zeros((8, wide), F32)
        for dj in range(2):
            for c in range(3):
                value = jnp.sum(
                    jnp.where(row_id == j_row + dj, found[c * rows : (c + 1) * rows], 0.0), axis=0, keepdims=True
                )
                out = jnp.where(sub == 4 * dj + c, value, out)
        eastern[dk] = out

    row_out.wait_recv()
    cnr_wait = remote(cnr, cnr_in, 2, 2, r, west)

    @pl.when(jnp.logical_or(jnp.logical_not(top), corner != p))
    def _():
        cnr_wait.wait_recv()

    @pl.when(jnp.logical_and(top, corner == p))
    def _():
        cfold_here.wait()

    northern = [[], []]
    corner_at = [
        jnp.dot(cnr_in[...].astype(BF16), at_level[dk], preferred_element_type=F32) for dk in range(2)
    ]
    col_id = iota((cols, LANES), 0)
    for t in range(tiles):
        part = slice(t * LANES, (t + 1) * LANES)
        hits = [col_id == first_col[:, part], col_id == second_col[:, part]]
        for dk in range(2):
            outs = [jnp.zeros((8, LANES), F32), jnp.zeros((8, LANES), F32)]
            for c in range(3):
                found = lax.dot_general(
                    nrow_in[:, c * cols : (c + 1) * cols], at_level[dk][0 : nrow_in.shape[0], part], TN,
                    preferred_element_type=F32,
                )
                for d in range(2):
                    value = jnp.sum(jnp.where(hits[d], found, 0.0), axis=0, keepdims=True)
                    outs[d] = jnp.where(iota((8, LANES), 0) == 4 + c, value, outs[d])
            northern[dk].append(outs)

    corners = [[None, None], [None, None]]
    lower = sub >= 4
    for dk in range(2):
        edge_value = pltpu.roll(corner_at[dk], 4, 0)
        for d in range(2):
            at_col = first_col if d == 0 else second_col
            north = jnp.concatenate([northern[dk][t][d] for t in range(tiles)], axis=1)
            north = sign * jnp.where(at_col == cols, edge_value, north)
            here = gathered[dk, d]
            if d == 1:
                here = jnp.where(i_row == cols - 1, eastern[dk], here)
            corners[dk][d] = jnp.where(lower & (j_row == rows - 1), north, here)

    posit[...] = jnp.zeros_like(posit)
    for n in range(3):
        posit[n : n + 1, :] = off_ref[n, :, 0:wide]
    position = posit[...]
    first = velocity_at(corners, position[0:1], position[1:2], position[2:3])
    middle = position + 0.5 * first
    moved = position + velocity_at(corners, middle[0:1], middle[1:2], middle[2:3])
    na, nb, nc = moved[0:1], moved[1:2], moved[2:3]
    new_a = jnp.where(
        motion == 1, na - 1.0, jnp.where(motion == 2, na + 1.0, jnp.where(folding, 1.0 - na, na))
    )
    new_b = jnp.where(
        motion == 3, jnp.where(top, 2.0 - nb, nb - 1.0), jnp.where(motion == 4, nb + 1.0, nb)
    )
    records = jnp.where(
        sub == 0, new_a, jnp.where(sub == 1, new_b, jnp.where(sub == 2, nc, jnp.where(sub == 3, code, 0.0)))
    )

    packets = placed(records, leave_to, 4 * LANES)
    for m in range(4):
        pack[m] = packets[:, m * LANES : (m + 1) * LANES]

    @pl.when(r == 0)
    def _():
        pack_in[2] = jnp.zeros((8, LANES), F32)

    east_out = remote(pack.at[0], pack_in.at[0], 5, 3, r, east)
    west_out = remote(pack.at[1], pack_in.at[1], 6, 4, r, west)
    north_out = remote(pack.at[2], pack_in.at[2], 7, 5, r + 1, p)
    over_out = remote(pack.at[2], pack_in.at[3], 7, 6, r, across)
    south_out = remote(pack.at[3], pack_in.at[3], 8, 6, r - 1, p)

    @pl.when(top)
    def _():
        over_out.start()

    @pl.when(r < n_lat - 1)
    def _():
        north_out.start()

    @pl.when(r > 0)
    def _():
        south_out.start()

    east_out.start()
    west_out.start()

    kept = placed(records, stay_to, wide)
    filled = total[0:1, :]

    east_out.wait_recv()
    west_out.wait_recv()

    @pl.when(r > 0)
    def _():
        north_out.wait_recv()

    over_out.wait_recv()

    arrivals = jnp.concatenate([pack_in[m] for m in range(4)], axis=1)
    lanes_row = iota((1, LANES), 1).astype(F32)
    targets = []
    for m in range(4):
        present = jnp.where(arrivals[3:4, m * LANES : (m + 1) * LANES] > 0.5, 1.0, 0.0)
        targets.append(jnp.where(present > 0.5, filled + lanes_row, -1.0))
        filled = filled + jnp.sum(present, axis=1, keepdims=True)
    joined = placed(arrivals, jnp.concatenate(targets, axis=1).astype(I32), slots)
    result = joined + jnp.concatenate([kept, jnp.zeros((8, slots - wide), F32)], axis=1)
    decoded = jnp.maximum(result[3:4].astype(I32) - 1, 0)
    for n in range(3):
        new_off[n] = result[n : n + 1]
    new_cell[0] = decoded & (cols - 1)
    new_cell[1] = (decoded // cols) & (rows - 1)
    new_cell[2] = decoded // (cols * rows)
    new_count[...] = filled[:, 0:1].astype(I32)

    ect_out.wait_send()
    east_out.wait_send()
    west_out.wait_send()
    north_out.wait_send()

    @pl.when(r > 0)
    def _():
        row_out.wait_send()
        cnr_out.wait_send()
        south_out.wait_send()

    @pl.when(top)
    def _():
        fold_out.wait_send()

    @pl.when(away)
    def _():
        cfold_out.wait_send()


def shards(velocity, offsets, cells, counts, moves):
    _, depth, rows, cols = velocity.shape
    slots = offsets.shape[2]
    live = slots * 3 // 4
    wide = pl.cdiv(live, LANES) * LANES
    deep = pl.cdiv(depth, 16) * 16
    dims = (depth, rows, cols, slots, live, lax.axis_size("lat"), lax.axis_size("lon"))
    vmem = pl.BlockSpec(memory_space=pltpu.VMEM)
    smem = pl.BlockSpec(memory_space=pltpu.SMEM)
    return pl.pallas_call(
        functools.partial(kernel, dims),
        out_shape=(
            jax.ShapeDtypeStruct((3, 1, slots), F32),
            jax.ShapeDtypeStruct((3, 1, slots), I32),
            jax.ShapeDtypeStruct((1, 1), I32),
        ),
        in_specs=[pl.BlockSpec(memory_space=pl.ANY), vmem, vmem, smem, smem, vmem],
        out_specs=(vmem, vmem, vmem),
        scratch_shapes=[
            pltpu.VMEM((3, depth, rows, cols), BF16),
            pltpu.VMEM((3 * deep * rows * 4, LANES), F32),
            pltpu.VMEM((2, 2, 8, wide), F32),
            pltpu.VMEM((8, wide), F32),
            pltpu.VMEM((3, rows, LANES), BF16),
            pltpu.VMEM((deep, 3 * cols), BF16),
            pltpu.VMEM((deep, 3 * cols), BF16),
            pltpu.VMEM((8, LANES), F32),
            pltpu.VMEM((8, LANES), F32),
            pltpu.VMEM((3, rows, LANES), BF16),
            pltpu.VMEM((deep, 3 * cols), BF16),
            pltpu.VMEM((8, LANES), F32),
            pltpu.VMEM((4, 8, LANES), F32),
            pltpu.VMEM((4, 8, LANES), F32),
            pltpu.SemaphoreType.DMA((3,)),
            pltpu.SemaphoreType.DMA((9,)),
            pltpu.SemaphoreType.DMA((7,)),
            pltpu.SemaphoreType.DMA,
        ],
        compiler_params=pltpu.CompilerParams(
            collective_id=0, has_side_effects=True, vmem_limit_bytes=48 * 1024 * 1024
        ),
        name="advance",
    )(velocity, offsets, cells, cells, counts, moves)


def solution(mesh):
    placed_in = (
        P(None, None, "lat", "lon"),
        P(None, "lat", "lon"),
        P(None, "lat", "lon"),
        P("lat", "lon"),
        P("lat", "lon"),
    )
    return jax.shard_map(
        shards,
        mesh=mesh,
        in_specs=placed_in,
        out_specs=(P(None, "lat", "lon"), P(None, "lat", "lon"), P("lat", "lon")),
        check_vma=False,
    )
```

```python
import functools

import jax
import jax.numpy as jnp
from jax import lax
from jax.experimental import pallas as pl
from jax.experimental.pallas import tpu as pltpu
from jax.sharding import PartitionSpec as P

MESH = pl.DeviceIdType.MESH
CAP = 48
LANES = 128
F32, BF16, I32 = jnp.float32, jnp.bfloat16, jnp.int32
NT = (((1,), (1,)), ((), ()))
TN = (((0,), (0,)), ((), ()))


def iota(shape, dim):
    return lax.broadcasted_iota(I32, shape, dim)


def thirds(x):
    high = x.astype(BF16)
    rest = x - high.astype(F32)
    mid = rest.astype(BF16)
    low = (rest - mid.astype(F32)).astype(BF16)
    return jnp.concatenate([high.astype(F32), mid.astype(F32), low.astype(F32)], axis=0).astype(BF16)


def slots_of(target, size):
    return jnp.where(iota((size, target.shape[1]), 0) == target, 1.0, 0.0).astype(BF16)


def placed(records, onehot):
    out = lax.dot_general(thirds(records), onehot, NT, preferred_element_type=F32)
    return out[0:8] + out[8:16] + out[16:24]


def velocity_at(corners, a_row, b_row, c_row):
    sub = iota((8, a_row.shape[1]), 0)
    wb = jnp.where(sub < 4, 1.0 - b_row, b_row)
    w0 = (wb * (1.0 - c_row)).astype(BF16).astype(F32)
    w1 = (wb * c_row).astype(BF16).astype(F32)
    sums = []
    for d in range(2):
        s = w0 * corners[0][d] + w1 * corners[1][d]
        sums.append(s + pltpu.roll(s, 4, 0))
    return (1.0 - a_row) * sums[0] + a_row * sums[1]


def kernel(
    dims, vel_hbm, off_hbm, cell_hbm, count_smem, move_hbm,
    new_off, new_cell, new_count,
    vel, off_ref, cell_ref, move_ref, table, where_ref, where_smem, gathered, posit, stay_ref, leave_ref,
    side, column, nrow, nfold, col_in, nrow_in, cnr_in,
    pack, pack_in, vsem, isem, send, recv, lsem, asem,
):
    depth, rows, cols, slots, live, n_lat, n_lon = dims
    wide = pl.cdiv(live, LANES) * LANES
    tiles = wide // LANES
    level = rows * 4
    span = table.shape[0] // 2
    per = LANES // rows
    groups = side.shape[1]
    r, p = lax.axis_index("lat"), lax.axis_index("lon")
    east, west = lax.rem(p + 1, n_lon), lax.rem(p + n_lon - 1, n_lon)
    across, corner = n_lon - 1 - p, lax.rem(n_lon - p, n_lon)
    top = r == n_lat - 1
    away = jnp.logical_and(top, corner != p)

    smalls = [(cell_hbm, cell_ref), (move_hbm, move_ref), (off_hbm, off_ref)]
    smalls = [pltpu.make_async_copy(src, dst, isem.at[n]) for n, (src, dst) in enumerate(smalls)]
    smalls[0].start()
    loads = [pltpu.make_async_copy(vel_hbm.at[c], vel.at[c], vsem.at[c]) for c in range(3)]
    for load in loads:
        load.start()
    for small in smalls[1:]:
        small.start()

    barrier = pltpu.get_barrier_semaphore()

    def greet(lat, lon):
        pl.semaphore_signal(barrier, inc=1, device_id=(lon, lat), device_id_type=MESH)

    greet(r, east)
    greet(r, west)

    @pl.when(r < n_lat - 1)
    def _():
        greet(r + 1, p)
        greet(r + 1, east)

    @pl.when(r > 0)
    def _():
        greet(r - 1, p)

    @pl.when(top)
    def _():
        greet(r, across)

    @pl.when(away)
    def _():
        greet(r, corner)

    lane = iota((8, LANES), 1)
    sub = iota((8, wide), 0)
    smalls[0].wait()
    i_row, j_row, k_row = (cell_ref[n, :, 0:wide] for n in range(3))
    start = jnp.where(i_row >= LANES, span, 0) + k_row * level + 4 * j_row
    start = start * LANES + ((iota((1, wide), 1) - i_row) & (LANES - 1))
    for t in range(tiles):
        part = start[:, t * LANES : (t + 1) * LANES]
        where_ref[2 * t : 2 * t + 1, :] = part
        where_ref[2 * t + 1 : 2 * t + 2, :] = pltpu.roll(part, LANES // 2, 1)
    addresses = pltpu.make_async_copy(where_ref, where_smem, asem)
    addresses.start()

    for part in range(2):
        table[pl.ds(part * span + depth * level, span - depth * level), :] = jnp.zeros(
            (span - depth * level, LANES), F32
        )
    side[...] = jnp.zeros_like(side)
    first_lane = jnp.where(lane == 0, 1.0, 0.0).astype(BF16)
    for c in range(3):
        loads[c].wait()

        def build(step, carry):
            for u in range(5):
                k = step * 5 + u
                for half in range(2):
                    plane = vel[c, k, :, half * LANES : (half + 1) * LANES].astype(F32)
                    for s in range(rows // 8):
                        at = half * span + k * level + 32 * s + c
                        table[pl.ds(at, 8, stride=4), :] = plane[8 * s : 8 * s + 8]
            return carry

        lax.fori_loop(0, depth // 5, build, 0)

        for half in range(2):
            plane = vel[c, :, :, half * LANES : (half + 1) * LANES].reshape(depth * rows, LANES)
            line = lax.dot_general(first_lane, plane, NT, preferred_element_type=F32)[0:1]
            for g in range(pl.cdiv(depth, per)):
                n = min(LANES, depth * rows - g * LANES)
                side[half * 3 + c, g : g + 1, 0:n] = line[:, g * LANES : g * LANES + n]
    column[...] = side[0:3].astype(BF16)

    def edge(target, row):
        for c in range(3):
            for half in range(2):
                for block in range(nrow.shape[0] // 16):
                    at = half * span + block * 16 * level + 4 * row + c
                    pair = [table[pl.ds(at + u * 8 * level, 8, stride=level), :] for u in range(2)]
                    target[pl.ds(block * 16, 16), pl.ds(c * cols + half * LANES, LANES)] = jnp.concatenate(
                        pair, axis=0
                    ).astype(BF16)

    edge(nrow, 0)

    @pl.when(top)
    def _():
        edge(nfold, rows - 1)

    def remote(src, dst, s, t, lat, lon):
        return pltpu.make_async_remote_copy(
            src, dst, send.at[s], recv.at[t], device_id=(lon, lat), device_id_type=MESH
        )

    col_out = remote(column, col_in, 0, 0, r, west)
    row_out = remote(nrow, nrow_in, 1, 1, r - 1, p)
    cnr_out = remote(column, cnr_in, 2, 2, r - 1, west)
    fold_out = remote(nfold, nrow_in, 3, 1, r, across)
    cfold_out = remote(column, cnr_in, 4, 2, r, corner)
    cfold_here = pltpu.make_async_copy(column, cnr_in, lsem)

    peers = 2 + 2 * (r > 0).astype(I32) + (r < n_lat - 1).astype(I32) + top.astype(I32) + away.astype(I32)
    pl.semaphore_wait(barrier, peers)

    @pl.when(r > 0)
    def _():
        row_out.start()
        cnr_out.start()

    @pl.when(top)
    def _():
        fold_out.start()

    @pl.when(away)
    def _():
        cfold_out.start()

    @pl.when(jnp.logical_and(top, corner == p))
    def _():
        cfold_here.start()

    col_out.start()

    gathered[...] = jnp.zeros_like(gathered)
    for small in smalls[1:]:
        small.wait()
    addresses.wait()
    half = LANES // 2

    def gather(step, carry):
        base = (step & 1) * half
        group = step // 2
        ahead = lane - base
        accs = [gathered[n, group] for n in range(4)]
        for u in range(half):
            word = where_smem[step, u]
            at, shift = word // LANES, word & (LANES - 1)
            here = ahead == u
            there = ahead == u + 1 if u < half - 1 else lane == ((base + half) & (LANES - 1))
            for dk in range(2):
                turned = pltpu.roll(table[pl.ds(at + dk * level, 8), :], shift, 1)
                accs[2 * dk] = jnp.where(here, turned, accs[2 * dk])
                accs[2 * dk + 1] = jnp.where(there, turned, accs[2 * dk + 1])
        for n in range(4):
            gathered[n, group] = accs[n]
        return carry

    lax.fori_loop(0, live // half, gather, 0)

    motion = move_ref[:, 0:wide]
    valid = iota((1, wide), 1) < count_smem[0, 0]
    chosen = jnp.where((sub == motion) & valid, 1.0, 0.0)
    before = jnp.where(iota((LANES, LANES), 0) < iota((LANES, LANES), 1), 1.0, 0.0).astype(BF16)
    upto = jnp.concatenate([before, jnp.ones((LANES, LANES), BF16)], axis=1)
    total = jnp.zeros((8, LANES), F32)
    ranks = []
    for t in range(tiles):
        sums = jnp.dot(
            chosen[:, t * LANES : (t + 1) * LANES].astype(BF16), upto, preferred_element_type=F32
        )
        ranks.append(sums[:, :LANES] + total)
        total = total + sums[:, LANES:]
    rank = jnp.concatenate(ranks, axis=1)
    stay_to = jnp.where(chosen[0:1] > 0.5, rank[0:1], -1.0).astype(I32)
    slot_to = rank + (LANES * (sub - 1)).astype(F32)
    leaving = (sub >= 1) & (chosen > 0.5)
    leave_to = (jnp.sum(jnp.where(leaving, slot_to + 1.0, 0.0), axis=0, keepdims=True) - 1.0).astype(I32)
    stay_ref[...] = slots_of(stay_to, wide)
    leave_ref[...] = slots_of(leave_to, 4 * LANES)
    folding = (motion == 3) & top
    last_i, last_j = cols - 1, rows - 1
    new_i = jnp.where(
        motion == 1, 0, jnp.where(motion == 2, last_i, jnp.where(folding, last_i - i_row, i_row))
    )
    new_j = jnp.where(
        motion == 3, jnp.where(top, last_j, 0), jnp.where(motion == 4, last_j, j_row)
    )
    code = (1 + new_i + cols * (new_j + rows * k_row)).astype(F32)
    posit[...] = jnp.zeros_like(posit)
    for n in range(3):
        posit[n : n + 1, :] = off_ref[n, :, 0:wide]

    deep = nrow_in.shape[0]
    both_k = jnp.concatenate([k_row, k_row + 1], axis=1)
    at_level = jnp.where(iota((deep, 2 * wide), 0) == both_k, 1.0, 0.0).astype(BF16)
    at_group = jnp.where(iota((groups, 2 * wide), 0) == both_k // per, 1.0, 0.0).astype(BF16)
    outer = jnp.concatenate([jnp.where(i_row == cols - 1, groups, 0)] * 2, axis=1)
    at_side = jnp.where(iota((2 * groups, 2 * wide), 0) == both_k // per + outer, 1.0, 0.0).astype(BF16)
    place = (both_k & (per - 1)) * rows + jnp.concatenate([j_row] * 2, axis=1)
    first_col = jnp.where(top, cols - i_row, i_row)
    second_col = jnp.where(top, cols - 1 - i_row, i_row + 1)
    sign = jnp.where(top, -1.0, 1.0)
    sub2 = iota((8, 2 * wide), 0)
    cnr_wait = remote(column, cnr_in, 2, 2, r, west)

    col_out.wait_recv()
    row_out.wait_recv()

    @pl.when(jnp.logical_or(jnp.logical_not(top), corner != p))
    def _():
        cnr_wait.wait_recv()

    @pl.when(jnp.logical_and(top, corner == p))
    def _():
        cfold_here.wait()

    eastern = jnp.zeros((8, 2 * wide), F32)
    lane_id = iota((LANES, 2 * wide), 0)
    hits = [lane_id == place + dj for dj in range(2)]
    for c in range(3):
        lines = jnp.concatenate([side[3 + c], col_in[c].astype(F32)], axis=0).astype(BF16)
        found = lax.dot_general(lines, at_side, TN, preferred_element_type=F32)
        for dj in range(2):
            value = jnp.sum(jnp.where(hits[dj], found, 0.0), axis=0, keepdims=True)
            eastern = jnp.where(sub2 == 4 * dj + c, value, eastern)

    edge_value = jnp.zeros((8, 2 * wide), F32)
    edge_lane = rows * iota((8, LANES), 0) + jnp.where(top, rows - 1, 0)
    pick = jnp.where(lane == edge_lane, 1.0, 0.0).astype(BF16)
    for c in range(3):
        few = lax.dot_general(pick, cnr_in[c], NT, preferred_element_type=F32).astype(BF16)
        found = jnp.dot(few, at_group, preferred_element_type=F32)
        value = jnp.sum(jnp.where(sub2 == (both_k & (per - 1)), found, 0.0), axis=0, keepdims=True)
        edge_value = jnp.where(sub2 == 4 + c, value, edge_value)

    northern = [jnp.zeros((8, 2 * wide), F32) for _ in range(2)]
    col_id = iota((cols, wide), 0)
    hits = [col_id == first_col, col_id == second_col]
    for c in range(3):
        found = lax.dot_general(
            nrow_in[:, c * cols : (c + 1) * cols], at_level, TN, preferred_element_type=F32
        )
        for d in range(2):
            value = jnp.concatenate(
                [
                    jnp.sum(
                        jnp.where(hits[d], found[:, dk * wide : (dk + 1) * wide], 0.0), axis=0, keepdims=True
                    )
                    for dk in range(2)
                ],
                axis=1,
            )
            northern[d] = jnp.where(sub2 == 4 + c, value, northern[d])

    corners = [[None, None], [None, None]]
    lower = sub >= 4
    for dk in range(2):
        part = slice(dk * wide, (dk + 1) * wide)
        for d in range(2):
            at_col = first_col if d == 0 else second_col
            north = sign * jnp.where(at_col == cols, edge_value[:, part], northern[d][:, part])
            inside = [gathered[2 * dk + d, t] for t in range(tiles)]
            if d == 1:
                inside = [pltpu.roll(x, LANES - 1, 1) for x in inside]
            inside = jnp.concatenate(inside, axis=1)
            if d == 1:
                inside = jnp.where((i_row & (LANES - 1)) == LANES - 1, eastern[:, part], inside)
            corners[dk][d] = jnp.where(lower & (j_row == rows - 1), north, inside)

    position = posit[...]
    first = velocity_at(corners, position[0:1], position[1:2], position[2:3])
    middle = position + 0.5 * first
    moved = position + velocity_at(corners, middle[0:1], middle[1:2], middle[2:3])
    na, nb, nc = moved[0:1], moved[1:2], moved[2:3]
    new_a = jnp.where(
        motion == 1, na - 1.0, jnp.where(motion == 2, na + 1.0, jnp.where(folding, 1.0 - na, na))
    )
    new_b = jnp.where(
        motion == 3, jnp.where(top, 2.0 - nb, nb - 1.0), jnp.where(motion == 4, nb + 1.0, nb)
    )
    records = jnp.where(
        sub == 0, new_a, jnp.where(sub == 1, new_b, jnp.where(sub == 2, nc, jnp.where(sub == 3, code, 0.0)))
    )

    packets = placed(records, leave_ref[...])
    for m in range(4):
        pack[m] = packets[:, m * LANES : (m + 1) * LANES]

    @pl.when(r == 0)
    def _():
        pack_in[2] = jnp.zeros((8, LANES), F32)

    east_out = remote(pack.at[0], pack_in.at[0], 5, 3, r, east)
    west_out = remote(pack.at[1], pack_in.at[1], 6, 4, r, west)
    north_out = remote(pack.at[2], pack_in.at[2], 7, 5, r + 1, p)
    over_out = remote(pack.at[2], pack_in.at[3], 7, 6, r, across)
    south_out = remote(pack.at[3], pack_in.at[3], 8, 6, r - 1, p)

    @pl.when(top)
    def _():
        over_out.start()

    @pl.when(r < n_lat - 1)
    def _():
        north_out.start()

    @pl.when(r > 0)
    def _():
        south_out.start()

    east_out.start()
    west_out.start()

    kept = placed(records, stay_ref[...])
    filled = total[0:1, :]

    east_out.wait_recv()
    west_out.wait_recv()

    @pl.when(r > 0)
    def _():
        north_out.wait_recv()

    over_out.wait_recv()

    arrivals = jnp.concatenate([pack_in[m] for m in range(4)], axis=1)
    lanes_row = iota((1, LANES), 1).astype(F32)
    targets = []
    for m in range(4):
        present = jnp.where(arrivals[3:4, m * LANES : (m + 1) * LANES] > 0.5, 1.0, 0.0)
        targets.append(jnp.where(present > 0.5, filled + lanes_row, -1.0))
        filled = filled + jnp.sum(present, axis=1, keepdims=True)
    joined = placed(arrivals, slots_of(jnp.concatenate(targets, axis=1).astype(I32), slots))
    result = joined + jnp.concatenate([kept, jnp.zeros((8, slots - wide), F32)], axis=1)
    decoded = jnp.maximum(result[3:4].astype(I32) - 1, 0)
    for n in range(3):
        new_off[n] = result[n : n + 1]
    new_cell[0] = decoded & (cols - 1)
    new_cell[1] = (decoded // cols) & (rows - 1)
    new_cell[2] = decoded // (cols * rows)
    new_count[...] = filled[:, 0:1].astype(I32)

    col_out.wait_send()
    east_out.wait_send()
    west_out.wait_send()
    north_out.wait_send()

    @pl.when(r > 0)
    def _():
        row_out.wait_send()
        cnr_out.wait_send()
        south_out.wait_send()

    @pl.when(top)
    def _():
        fold_out.wait_send()

    @pl.when(away)
    def _():
        cfold_out.wait_send()


def shards(velocity, offsets, cells, counts, moves):
    _, depth, rows, cols = velocity.shape
    slots = offsets.shape[2]
    live = slots * 3 // 4
    wide = pl.cdiv(live, LANES) * LANES
    deep = pl.cdiv(depth, 16) * 16
    dims = (depth, rows, cols, slots, live, lax.axis_size("lat"), lax.axis_size("lon"))
    groups = pl.cdiv(depth * rows, 8 * LANES) * 8
    vmem = pl.BlockSpec(memory_space=pltpu.VMEM)
    hbm = pl.BlockSpec(memory_space=pl.ANY)
    return pl.pallas_call(
        functools.partial(kernel, dims),
        out_shape=(
            jax.ShapeDtypeStruct((3, 1, slots), F32),
            jax.ShapeDtypeStruct((3, 1, slots), I32),
            jax.ShapeDtypeStruct((1, 1), I32),
        ),
        in_specs=[hbm, hbm, hbm, pl.BlockSpec(memory_space=pltpu.SMEM), hbm],
        out_specs=(vmem, vmem, vmem),
        scratch_shapes=[
            pltpu.VMEM((3, depth, rows, cols), BF16),
            pltpu.VMEM((3, 1, slots), F32),
            pltpu.VMEM((3, 1, slots), I32),
            pltpu.VMEM((1, slots), I32),
            pltpu.VMEM((2 * deep * rows * 4, LANES), F32),
            pltpu.VMEM((2 * wide // LANES, LANES), I32),
            pltpu.SMEM((2 * wide // LANES, LANES), I32),
            pltpu.VMEM((4, wide // LANES, 8, LANES), F32),
            pltpu.VMEM((8, wide), F32),
            pltpu.VMEM((wide, wide), BF16),
            pltpu.VMEM((4 * LANES, wide), BF16),
            pltpu.VMEM((6, groups, LANES), F32),
            pltpu.VMEM((3, groups, LANES), BF16),
            pltpu.VMEM((deep, 3 * cols), BF16),
            pltpu.VMEM((deep, 3 * cols), BF16),
            pltpu.VMEM((3, groups, LANES), BF16),
            pltpu.VMEM((deep, 3 * cols), BF16),
            pltpu.VMEM((3, groups, LANES), BF16),
            pltpu.VMEM((4, 8, LANES), F32),
            pltpu.VMEM((4, 8, LANES), F32),
            pltpu.SemaphoreType.DMA((3,)),
            pltpu.SemaphoreType.DMA((3,)),
            pltpu.SemaphoreType.DMA((9,)),
            pltpu.SemaphoreType.DMA((7,)),
            pltpu.SemaphoreType.DMA,
            pltpu.SemaphoreType.DMA,
        ],
        compiler_params=pltpu.CompilerParams(
            collective_id=0, has_side_effects=True, vmem_limit_bytes=67043328
        ),
        name="advance",
    )(velocity, offsets, cells, counts, moves)


def solution(mesh):
    placed_in = (
        P(None, None, "lat", "lon"),
        P(None, "lat", "lon"),
        P(None, "lat", "lon"),
        P("lat", "lon"),
        P("lat", "lon"),
    )
    return jax.shard_map(
        shards,
        mesh=mesh,
        in_specs=placed_in,
        out_specs=(P(None, "lat", "lon"), P(None, "lat", "lon"), P("lat", "lon")),
        check_vma=False,
    )
```

```python
import functools

import jax
import jax.numpy as jnp
from jax import lax
from jax.experimental import pallas as pl
from jax.experimental.pallas import tpu as pltpu
from jax.sharding import PartitionSpec as P

MESH = pl.DeviceIdType.MESH
CAP = 48
LANES = 128
F32, BF16, I32 = jnp.float32, jnp.bfloat16, jnp.int32
NT = (((1,), (1,)), ((), ()))
TN = (((0,), (0,)), ((), ()))


def iota(shape, dim):
    return lax.broadcasted_iota(I32, shape, dim)


def thirds(x):
    high = x.astype(BF16)
    rest = x - high.astype(F32)
    mid = rest.astype(BF16)
    low = (rest - mid.astype(F32)).astype(BF16)
    return jnp.concatenate([high.astype(F32), mid.astype(F32), low.astype(F32)], axis=0).astype(BF16)


def slots_of(target, size):
    return jnp.where(iota((size, target.shape[1]), 0) == target, 1.0, 0.0).astype(BF16)


def placed(records, onehot):
    out = lax.dot_general(thirds(records), onehot, NT, preferred_element_type=F32)
    return out[0:8] + out[8:16] + out[16:24]


def velocity_at(corners, a_row, b_row, c_row):
    sub = iota((8, a_row.shape[1]), 0)
    wb = jnp.where(sub < 4, 1.0 - b_row, b_row)
    w0 = (wb * (1.0 - c_row)).astype(BF16).astype(F32)
    w1 = (wb * c_row).astype(BF16).astype(F32)
    sums = []
    for d in range(2):
        s = w0 * corners[0][d] + w1 * corners[1][d]
        sums.append(s + pltpu.roll(s, 4, 0))
    return (1.0 - a_row) * sums[0] + a_row * sums[1]


def kernel(
    dims, vel_hbm, off_hbm, cell_hbm, count_hbm, move_hbm,
    out_ref,
    vel, off_ref, cell_ref, move_ref, count_ref, table, where_ref, where_smem, gathered, posit, stay_ref, leave_ref,
    side, column, nrow, nfold, col_in, nrow_in, cnr_in,
    pack, pack_in, vsem, isem, send, recv, lsem, asem,
):
    depth, rows, cols, slots, live, n_lat, n_lon = dims
    wide = pl.cdiv(live, LANES) * LANES
    tiles = wide // LANES
    level = rows * 4
    span = table.shape[0] // 2
    per = LANES // rows
    groups = side.shape[1]
    r, p = lax.axis_index("lat"), lax.axis_index("lon")
    east, west = lax.rem(p + 1, n_lon), lax.rem(p + n_lon - 1, n_lon)
    across, corner = n_lon - 1 - p, lax.rem(n_lon - p, n_lon)
    top = r == n_lat - 1
    away = jnp.logical_and(top, corner != p)

    smalls = [(cell_hbm, cell_ref), (move_hbm, move_ref), (count_hbm, count_ref), (off_hbm, off_ref)]
    smalls = [pltpu.make_async_copy(src, dst, isem.at[n]) for n, (src, dst) in enumerate(smalls)]
    smalls[0].start()
    loads = [pltpu.make_async_copy(vel_hbm.at[c], vel.at[c], vsem.at[c]) for c in range(3)]
    for load in loads:
        load.start()
    for small in smalls[1:]:
        small.start()

    barrier = pltpu.get_barrier_semaphore()

    def greet(lat, lon):
        pl.semaphore_signal(barrier, inc=1, device_id=(lon, lat), device_id_type=MESH)

    greet(r, east)
    greet(r, west)

    @pl.when(r < n_lat - 1)
    def _():
        greet(r + 1, p)
        greet(r + 1, east)

    @pl.when(r > 0)
    def _():
        greet(r - 1, p)

    @pl.when(top)
    def _():
        greet(r, across)

    @pl.when(away)
    def _():
        greet(r, corner)

    lane = iota((8, LANES), 1)
    sub = iota((8, wide), 0)
    smalls[0].wait()
    i_row, j_row, k_row = (cell_ref[n, :, 0:wide] for n in range(3))
    start = jnp.where(i_row >= LANES, span, 0) + k_row * level + 4 * j_row
    start = start * LANES + ((iota((1, wide), 1) - i_row) & (LANES - 1))
    for t in range(tiles):
        part = start[:, t * LANES : (t + 1) * LANES]
        where_ref[2 * t : 2 * t + 1, :] = part
        where_ref[2 * t + 1 : 2 * t + 2, :] = pltpu.roll(part, LANES // 2, 1)
    addresses = pltpu.make_async_copy(where_ref, where_smem, asem)
    addresses.start()

    for part in range(2):
        table[pl.ds(part * span + depth * level, span - depth * level), :] = jnp.zeros(
            (span - depth * level, LANES), F32
        )
    side[...] = jnp.zeros_like(side)
    first_lane = jnp.where(lane == 0, 1.0, 0.0).astype(BF16)
    for c in range(3):
        loads[c].wait()

        def build(step, carry):
            for u in range(5):
                k = step * 5 + u
                for half in range(2):
                    plane = vel[c, k, :, half * LANES : (half + 1) * LANES].astype(F32)
                    for s in range(rows // 8):
                        at = half * span + k * level + 32 * s + c
                        table[pl.ds(at, 8, stride=4), :] = plane[8 * s : 8 * s + 8]
            return carry

        lax.fori_loop(0, depth // 5, build, 0)

        for half in range(2):
            plane = vel[c, :, :, half * LANES : (half + 1) * LANES].reshape(depth * rows, LANES)
            line = lax.dot_general(first_lane, plane, NT, preferred_element_type=F32)[0:1]
            for g in range(pl.cdiv(depth, per)):
                n = min(LANES, depth * rows - g * LANES)
                side[half * 3 + c, g : g + 1, 0:n] = line[:, g * LANES : g * LANES + n]
    column[...] = side[0:3].astype(BF16)

    def edge(target, row):
        for c in range(3):
            for half in range(2):
                for block in range(nrow.shape[0] // 16):
                    at = half * span + block * 16 * level + 4 * row + c
                    pair = [table[pl.ds(at + u * 8 * level, 8, stride=level), :] for u in range(2)]
                    target[pl.ds(block * 16, 16), pl.ds(c * cols + half * LANES, LANES)] = jnp.concatenate(
                        pair, axis=0
                    ).astype(BF16)

    edge(nrow, 0)

    @pl.when(top)
    def _():
        edge(nfold, rows - 1)

    def remote(src, dst, s, t, lat, lon):
        return pltpu.make_async_remote_copy(
            src, dst, send.at[s], recv.at[t], device_id=(lon, lat), device_id_type=MESH
        )

    col_out = remote(column, col_in, 0, 0, r, west)
    row_out = remote(nrow, nrow_in, 1, 1, r - 1, p)
    cnr_out = remote(column, cnr_in, 2, 2, r - 1, west)
    fold_out = remote(nfold, nrow_in, 3, 1, r, across)
    cfold_out = remote(column, cnr_in, 4, 2, r, corner)
    cfold_here = pltpu.make_async_copy(column, cnr_in, lsem)

    peers = 2 + 2 * (r > 0).astype(I32) + (r < n_lat - 1).astype(I32) + top.astype(I32) + away.astype(I32)
    pl.semaphore_wait(barrier, peers)

    @pl.when(r > 0)
    def _():
        row_out.start()
        cnr_out.start()

    @pl.when(top)
    def _():
        fold_out.start()

    @pl.when(away)
    def _():
        cfold_out.start()

    @pl.when(jnp.logical_and(top, corner == p))
    def _():
        cfold_here.start()

    col_out.start()

    gathered[...] = jnp.zeros_like(gathered)
    for small in smalls[1:]:
        small.wait()
    addresses.wait()
    half = LANES // 2

    def gather(step, carry):
        base = (step & 1) * half
        group = step >> 1
        ahead = lane - base
        accs = [gathered[n, group] for n in range(4)]
        for u in range(half):
            word = where_smem[step, u]
            at, shift = word >> 7, word & (LANES - 1)
            here = ahead == u
            there = ahead == u + 1 if u < half - 1 else lane == ((base + half) & (LANES - 1))
            for dk in range(2):
                turned = pltpu.roll(table[pl.ds(at + dk * level, 8), :], shift, 1)
                accs[2 * dk] = jnp.where(here, turned, accs[2 * dk])
                accs[2 * dk + 1] = jnp.where(there, turned, accs[2 * dk + 1])
        for n in range(4):
            gathered[n, group] = accs[n]
        return carry

    lax.fori_loop(0, live // half, gather, 0)

    motion = move_ref[:, 0:wide]
    valid = iota((1, wide), 1) < count_ref[...]
    chosen = jnp.where((sub == motion) & valid, 1.0, 0.0)
    before = jnp.where(iota((LANES, LANES), 0) < iota((LANES, LANES), 1), 1.0, 0.0).astype(BF16)
    upto = jnp.concatenate([before, jnp.ones((LANES, LANES), BF16)], axis=1)
    total = jnp.zeros((8, LANES), F32)
    ranks = []
    for t in range(tiles):
        sums = jnp.dot(
            chosen[:, t * LANES : (t + 1) * LANES].astype(BF16), upto, preferred_element_type=F32
        )
        ranks.append(sums[:, :LANES] + total)
        total = total + sums[:, LANES:]
    rank = jnp.concatenate(ranks, axis=1)
    stay_to = jnp.where(chosen[0:1] > 0.5, rank[0:1], -1.0).astype(I32)
    slot_to = rank + (LANES * (sub - 1)).astype(F32)
    leaving = (sub >= 1) & (chosen > 0.5)
    leave_to = (jnp.sum(jnp.where(leaving, slot_to + 1.0, 0.0), axis=0, keepdims=True) - 1.0).astype(I32)
    stay_ref[...] = slots_of(stay_to, wide)
    leave_ref[...] = slots_of(leave_to, 4 * LANES)
    folding = (motion == 3) & top
    last_i, last_j = cols - 1, rows - 1
    new_i = jnp.where(
        motion == 1, 0, jnp.where(motion == 2, last_i, jnp.where(folding, last_i - i_row, i_row))
    )
    new_j = jnp.where(
        motion == 3, jnp.where(top, last_j, 0), jnp.where(motion == 4, last_j, j_row)
    )
    code = (1 + new_i + cols * (new_j + rows * k_row)).astype(F32)
    posit[...] = jnp.zeros_like(posit)
    for n in range(3):
        posit[n : n + 1, :] = off_ref[n, :, 0:wide]

    deep = nrow_in.shape[0]
    both_k = jnp.concatenate([k_row, k_row + 1], axis=1)
    at_level = jnp.where(iota((deep, 2 * wide), 0) == both_k, 1.0, 0.0).astype(BF16)
    at_group = jnp.where(iota((groups, 2 * wide), 0) == both_k // per, 1.0, 0.0).astype(BF16)
    outer = jnp.concatenate([jnp.where(i_row == cols - 1, groups, 0)] * 2, axis=1)
    at_side = jnp.where(iota((2 * groups, 2 * wide), 0) == both_k // per + outer, 1.0, 0.0).astype(BF16)
    place = (both_k & (per - 1)) * rows + jnp.concatenate([j_row] * 2, axis=1)
    first_col = jnp.where(top, cols - i_row, i_row)
    second_col = jnp.where(top, cols - 1 - i_row, i_row + 1)
    sign = jnp.where(top, -1.0, 1.0)
    sub2 = iota((8, 2 * wide), 0)
    cnr_wait = remote(column, cnr_in, 2, 2, r, west)

    col_out.wait_recv()
    row_out.wait_recv()

    @pl.when(jnp.logical_or(jnp.logical_not(top), corner != p))
    def _():
        cnr_wait.wait_recv()

    @pl.when(jnp.logical_and(top, corner == p))
    def _():
        cfold_here.wait()

    eastern = jnp.zeros((8, 2 * wide), F32)
    lane_id = iota((LANES, 2 * wide), 0)
    hits = [lane_id == place + dj for dj in range(2)]
    for c in range(3):
        lines = jnp.concatenate([side[3 + c], col_in[c].astype(F32)], axis=0).astype(BF16)
        found = lax.dot_general(lines, at_side, TN, preferred_element_type=F32)
        for dj in range(2):
            value = jnp.sum(jnp.where(hits[dj], found, 0.0), axis=0, keepdims=True)
            eastern = jnp.where(sub2 == 4 * dj + c, value, eastern)

    edge_value = jnp.zeros((8, 2 * wide), F32)
    edge_lane = rows * iota((8, LANES), 0) + jnp.where(top, rows - 1, 0)
    pick = jnp.where(lane == edge_lane, 1.0, 0.0).astype(BF16)
    for c in range(3):
        few = lax.dot_general(pick, cnr_in[c], NT, preferred_element_type=F32).astype(BF16)
        found = jnp.dot(few, at_group, preferred_element_type=F32)
        value = jnp.sum(jnp.where(sub2 == (both_k & (per - 1)), found, 0.0), axis=0, keepdims=True)
        edge_value = jnp.where(sub2 == 4 + c, value, edge_value)

    northern = [jnp.zeros((8, 2 * wide), F32) for _ in range(2)]
    col_id = iota((cols, wide), 0)
    hits = [col_id == first_col, col_id == second_col]
    for c in range(3):
        found = lax.dot_general(
            nrow_in[:, c * cols : (c + 1) * cols], at_level, TN, preferred_element_type=F32
        )
        for d in range(2):
            value = jnp.concatenate(
                [
                    jnp.sum(
                        jnp.where(hits[d], found[:, dk * wide : (dk + 1) * wide], 0.0), axis=0, keepdims=True
                    )
                    for dk in range(2)
                ],
                axis=1,
            )
            northern[d] = jnp.where(sub2 == 4 + c, value, northern[d])

    corners = [[None, None], [None, None]]
    lower = sub >= 4
    for dk in range(2):
        part = slice(dk * wide, (dk + 1) * wide)
        for d in range(2):
            at_col = first_col if d == 0 else second_col
            north = sign * jnp.where(at_col == cols, edge_value[:, part], northern[d][:, part])
            inside = [gathered[2 * dk + d, t] for t in range(tiles)]
            if d == 1:
                inside = [pltpu.roll(x, LANES - 1, 1) for x in inside]
            inside = jnp.concatenate(inside, axis=1)
            if d == 1:
                inside = jnp.where((i_row & (LANES - 1)) == LANES - 1, eastern[:, part], inside)
            corners[dk][d] = jnp.where(lower & (j_row == rows - 1), north, inside)

    position = posit[...]
    first = velocity_at(corners, position[0:1], position[1:2], position[2:3])
    middle = position + 0.5 * first
    moved = position + velocity_at(corners, middle[0:1], middle[1:2], middle[2:3])
    na, nb, nc = moved[0:1], moved[1:2], moved[2:3]
    new_a = jnp.where(
        motion == 1, na - 1.0, jnp.where(motion == 2, na + 1.0, jnp.where(folding, 1.0 - na, na))
    )
    new_b = jnp.where(
        motion == 3, jnp.where(top, 2.0 - nb, nb - 1.0), jnp.where(motion == 4, nb + 1.0, nb)
    )
    records = jnp.where(
        sub == 0, new_a, jnp.where(sub == 1, new_b, jnp.where(sub == 2, nc, jnp.where(sub == 3, code, 0.0)))
    )

    packets = placed(records, leave_ref[...])
    for m in range(4):
        pack[m] = packets[:, m * LANES : (m + 1) * LANES]

    @pl.when(r == 0)
    def _():
        pack_in[2] = jnp.zeros((8, LANES), F32)

    east_out = remote(pack.at[0], pack_in.at[0], 5, 3, r, east)
    west_out = remote(pack.at[1], pack_in.at[1], 6, 4, r, west)
    north_out = remote(pack.at[2], pack_in.at[2], 7, 5, r + 1, p)
    over_out = remote(pack.at[2], pack_in.at[3], 7, 6, r, across)
    south_out = remote(pack.at[3], pack_in.at[3], 8, 6, r - 1, p)

    @pl.when(top)
    def _():
        over_out.start()

    @pl.when(r < n_lat - 1)
    def _():
        north_out.start()

    @pl.when(r > 0)
    def _():
        south_out.start()

    east_out.start()
    west_out.start()

    kept = placed(records, stay_ref[...])
    filled = total[0:1, :]

    east_out.wait_recv()
    west_out.wait_recv()

    @pl.when(r > 0)
    def _():
        north_out.wait_recv()

    over_out.wait_recv()

    arrivals = jnp.concatenate([pack_in[m] for m in range(4)], axis=1)
    lanes_row = iota((1, LANES), 1).astype(F32)
    targets = []
    for m in range(4):
        present = jnp.where(arrivals[3:4, m * LANES : (m + 1) * LANES] > 0.5, 1.0, 0.0)
        targets.append(jnp.where(present > 0.5, filled + lanes_row, -1.0))
        filled = filled + jnp.sum(present, axis=1, keepdims=True)
    joined = placed(arrivals, slots_of(jnp.concatenate(targets, axis=1).astype(I32), slots))
    result = joined + jnp.concatenate([kept, jnp.zeros((8, slots - wide), F32)], axis=1)
    out_ref[...] = jnp.where(iota((8, slots), 0) == 4, filled[:, 0:1], result)

    col_out.wait_send()
    east_out.wait_send()
    west_out.wait_send()
    north_out.wait_send()

    @pl.when(r > 0)
    def _():
        row_out.wait_send()
        cnr_out.wait_send()
        south_out.wait_send()

    @pl.when(top)
    def _():
        fold_out.wait_send()

    @pl.when(away)
    def _():
        cfold_out.wait_send()


def decode(rows, cols, result_ref, new_off, new_cell, new_count):
    for n in range(3):
        new_off[n] = result_ref[n : n + 1, :]
    code = jnp.maximum(result_ref[3:4, :].astype(I32) - 1, 0)
    new_cell[0] = code & (cols - 1)
    new_cell[1] = (code // cols) & (rows - 1)
    new_cell[2] = code // (cols * rows)
    new_count[...] = result_ref[4:5, 0:1].astype(I32)


def shards(velocity, offsets, cells, counts, moves):
    _, depth, rows, cols = velocity.shape
    slots = offsets.shape[2]
    live = slots * 3 // 4
    wide = pl.cdiv(live, LANES) * LANES
    deep = pl.cdiv(depth, 16) * 16
    dims = (depth, rows, cols, slots, live, lax.axis_size("lat"), lax.axis_size("lon"))
    groups = pl.cdiv(depth * rows, 8 * LANES) * 8
    vmem = pl.BlockSpec(memory_space=pltpu.VMEM)
    hbm = pl.BlockSpec(memory_space=pltpu.HBM)
    velocity, offsets, cells, moves = (
        pltpu.with_memory_space_constraint(x, pltpu.HBM) for x in (velocity, offsets, cells, moves)
    )
    result = pl.pallas_call(
        functools.partial(kernel, dims),
        out_shape=jax.ShapeDtypeStruct((8, slots), F32),
        in_specs=[hbm] * 5,
        out_specs=vmem,
        scratch_shapes=[
            pltpu.VMEM((3, depth, rows, cols), BF16),
            pltpu.VMEM((3, 1, slots), F32),
            pltpu.VMEM((3, 1, slots), I32),
            pltpu.VMEM((1, slots), I32),
            pltpu.VMEM((1, 1), I32),
            pltpu.VMEM((2 * deep * rows * 4, LANES), F32),
            pltpu.VMEM((2 * wide // LANES, LANES), I32),
            pltpu.SMEM((2 * wide // LANES, LANES), I32),
            pltpu.VMEM((4, wide // LANES, 8, LANES), F32),
            pltpu.VMEM((8, wide), F32),
            pltpu.VMEM((wide, wide), BF16),
            pltpu.VMEM((4 * LANES, wide), BF16),
            pltpu.VMEM((6, groups, LANES), F32),
            pltpu.VMEM((3, groups, LANES), BF16),
            pltpu.VMEM((deep, 3 * cols), BF16),
            pltpu.VMEM((deep, 3 * cols), BF16),
            pltpu.VMEM((3, groups, LANES), BF16),
            pltpu.VMEM((deep, 3 * cols), BF16),
            pltpu.VMEM((3, groups, LANES), BF16),
            pltpu.VMEM((4, 8, LANES), F32),
            pltpu.VMEM((4, 8, LANES), F32),
            pltpu.SemaphoreType.DMA((3,)),
            pltpu.SemaphoreType.DMA((4,)),
            pltpu.SemaphoreType.DMA((9,)),
            pltpu.SemaphoreType.DMA((7,)),
            pltpu.SemaphoreType.DMA,
            pltpu.SemaphoreType.DMA,
        ],
        compiler_params=pltpu.CompilerParams(
            collective_id=0, has_side_effects=True, vmem_limit_bytes=32 * 1024 * 1024
        ),
        name="advance",
    )(velocity, offsets, cells, counts, moves)
    return pl.pallas_call(
        functools.partial(decode, rows, cols),
        out_shape=(
            jax.ShapeDtypeStruct((3, 1, slots), F32),
            jax.ShapeDtypeStruct((3, 1, slots), I32),
            jax.ShapeDtypeStruct((1, 1), I32),
        ),
        in_specs=[vmem],
        out_specs=(vmem, vmem, vmem),
        compiler_params=pltpu.CompilerParams(vmem_limit_bytes=1024 * 1024),
        name="decode",
    )(result)


def solution(mesh):
    placed_in = (
        P(None, None, "lat", "lon"),
        P(None, "lat", "lon"),
        P(None, "lat", "lon"),
        P("lat", "lon"),
        P("lat", "lon"),
    )
    return jax.shard_map(
        shards,
        mesh=mesh,
        in_specs=placed_in,
        out_specs=(P(None, "lat", "lon"), P(None, "lat", "lon"), P("lat", "lon")),
        check_vma=False,
    )
```

```python
import functools

import jax
import jax.numpy as jnp
from jax import lax
from jax.experimental import pallas as pl
from jax.experimental.pallas import tpu as pltpu
from jax.sharding import PartitionSpec as P

MESH = pl.DeviceIdType.MESH
CAP = 48
LANES = 128
F32, BF16, I32 = jnp.float32, jnp.bfloat16, jnp.int32
NT = (((1,), (1,)), ((), ()))
TN = (((0,), (0,)), ((), ()))


def iota(shape, dim):
    return lax.broadcasted_iota(I32, shape, dim)


def thirds(x):
    high = x.astype(BF16)
    rest = x - high.astype(F32)
    mid = rest.astype(BF16)
    low = (rest - mid.astype(F32)).astype(BF16)
    return jnp.concatenate([high.astype(F32), mid.astype(F32), low.astype(F32)], axis=0).astype(BF16)


def slots_of(target, size):
    return jnp.where(iota((size, target.shape[1]), 0) == target, 1.0, 0.0).astype(BF16)


def placed(records, onehot):
    out = lax.dot_general(thirds(records), onehot, NT, preferred_element_type=F32)
    return out[0:8] + out[8:16] + out[16:24]


def velocity_at(corners, a_row, b_row, c_row):
    sub = iota((8, a_row.shape[1]), 0)
    wb = jnp.where(sub < 4, 1.0 - b_row, b_row)
    w0 = (wb * (1.0 - c_row)).astype(BF16).astype(F32)
    w1 = (wb * c_row).astype(BF16).astype(F32)
    sums = []
    for d in range(2):
        s = w0 * corners[0][d] + w1 * corners[1][d]
        sums.append(s + pltpu.roll(s, 4, 0))
    return (1.0 - a_row) * sums[0] + a_row * sums[1]


def halo_corners(w, i_row, j_row, k_row, inside, top, sides, nrow_in, cnr_in):
    cols, rows = 2 * LANES, sides[0].shape[0]
    deep = (nrow_in.shape[0] - 16) // 2
    groups = sides[0].shape[1] // 8
    per = LANES // rows
    sub2 = iota((8, 2 * w), 0)

    def twice(x):
        return jnp.concatenate([x] * 2, axis=1)

    def hot(size, at):
        return jnp.where(iota((size, 2 * w), 0) == at, 1.0, 0.0).astype(BF16)

    k2 = jnp.concatenate([k_row, k_row + 1], axis=1)
    j2 = twice(j_row)
    outer = twice(jnp.where(i_row == cols - 1, groups, 0))
    at_side = hot(8 * groups, (k2 & (per - 1)) * (2 * groups) + outer + lax.shift_right_logical(k2, per.bit_length() - 1))
    base = twice(jnp.where(top, cols - 1 - i_row, i_row))
    second = base >= LANES
    inner = base & (LANES - 1)
    at_row = hot(2 * deep, k2 + jnp.where(second, deep, 0))
    at_level = hot(LANES, k2)

    eastern = jnp.zeros((8, 2 * w), F32)
    hits = [iota((rows, 2 * w), 0) == j2 + dj for dj in range(2)]
    for c in range(3):
        found = jnp.dot(sides[c], at_side, preferred_element_type=F32)
        for dj in range(2):
            value = jnp.sum(jnp.where(hits[dj], found, 0.0), axis=0, keepdims=True)
            eastern = jnp.where(sub2 == 4 * dj + c, value, eastern)

    few = jnp.concatenate([cnr_in[...], nrow_in[2 * deep :, 0:LANES].astype(F32)], axis=0).astype(BF16)
    ends = jnp.dot(few, at_level, preferred_element_type=F32)
    last = pltpu.roll(jnp.where(second, ends[0:8], ends[8:16]), 4, 0)

    pair = [jnp.zeros((8, 2 * w), F32), last]
    lane_id = iota((LANES, 2 * w), 0)
    hits = [lane_id == inner, lane_id == inner + 1]
    for c in range(3):
        found = lax.dot_general(
            nrow_in[0 : 2 * deep, c * LANES : (c + 1) * LANES], at_row, TN, preferred_element_type=F32
        )
        for d in range(2):
            value = jnp.sum(jnp.where(hits[d], found, 0.0), axis=0, keepdims=True)
            put = sub2 == 4 + c
            pair[d] = jnp.where(put & (inner < LANES - 1) if d else put, value, pair[d])

    sign = jnp.where(top, -1.0, 1.0)
    north = [sign * jnp.where(top, pair[1 - d], pair[d]) for d in range(2)]
    lower = iota((8, w), 0) >= 4
    corners = []
    for dk in range(2):
        part = slice(dk * w, (dk + 1) * w)
        out = []
        for d in range(2):
            here = inside[dk][d]
            if d == 1:
                here = jnp.where((i_row & (LANES - 1)) == LANES - 1, eastern[:, part], here)
            out.append(jnp.where(lower & (j_row == rows - 1), north[d][:, part], here))
        corners.append(out)
    return corners


def advanced(corners, position):
    first = velocity_at(corners, position[0:1], position[1:2], position[2:3])
    middle = position + 0.5 * first
    return position + velocity_at(corners, middle[0:1], middle[1:2], middle[2:3])


def kernel(
    dims, vel_hbm, off_hbm, cell_hbm, count_hbm, move_hbm,
    out_ref,
    vel, off_ref, cell_ref, move_ref, count_ref, table, where_ref, where_smem, first_ref, first_smem,
    gathered, first_gathered, stay_ref,
    side, column, nrow, nfold, cnr, cfold, col_in, nrow_in, cnr_in,
    pack, pack_in, vsem, isem, send, recv, lsem, asem,
):
    depth, rows, cols, slots, live, n_lat, n_lon = dims
    wide = pl.cdiv(live, LANES) * LANES
    tiles = wide // LANES
    half = LANES // 2
    few = 4 * half
    level = rows * 4
    span = table.shape[0] // 2
    deep = span // level
    per = LANES // rows
    groups = side.shape[1]
    r, p = lax.axis_index("lat"), lax.axis_index("lon")
    east, west = lax.rem(p + 1, n_lon), lax.rem(p + n_lon - 1, n_lon)
    across, corner = n_lon - 1 - p, lax.rem(n_lon - p, n_lon)
    top = r == n_lat - 1
    away = jnp.logical_and(top, corner != p)

    smalls = [(cell_hbm, cell_ref), (move_hbm, move_ref), (count_hbm, count_ref), (off_hbm, off_ref)]
    smalls = [pltpu.make_async_copy(src, dst, isem.at[n]) for n, (src, dst) in enumerate(smalls)]
    for small in smalls:
        small.start()
    loads = [pltpu.make_async_copy(vel_hbm.at[c], vel.at[c], vsem.at[c]) for c in range(3)]
    for load in loads:
        load.start()

    barrier = pltpu.get_barrier_semaphore()

    def greet(lat, lon):
        pl.semaphore_signal(barrier, inc=1, device_id=(lon, lat), device_id_type=MESH)

    greet(r, east)
    greet(r, west)

    @pl.when(r < n_lat - 1)
    def _():
        greet(r + 1, p)
        greet(r + 1, east)

    @pl.when(r > 0)
    def _():
        greet(r - 1, p)

    @pl.when(top)
    def _():
        greet(r, across)

    @pl.when(away)
    def _():
        greet(r, corner)

    lane = iota((8, LANES), 1)
    sub = iota((8, wide), 0)
    for small in smalls:
        small.wait()

    i_row, j_row, k_row = (cell_ref[n, :, 0:wide] for n in range(3))
    motion = move_ref[:, 0:wide]
    valid = iota((1, wide), 1) < count_ref[...]
    chosen = jnp.where((sub == motion) & valid, 1.0, 0.0)
    before = jnp.where(iota((LANES, LANES), 0) < iota((LANES, LANES), 1), 1.0, 0.0).astype(BF16)
    upto = jnp.concatenate([before, jnp.ones((LANES, LANES), BF16)], axis=1)

    def ranked(flags, total):
        out = []
        for t in range(flags.shape[1] // LANES):
            sums = jnp.dot(
                flags[:, t * LANES : (t + 1) * LANES].astype(BF16), upto, preferred_element_type=F32
            )
            out.append(sums[:, :LANES] + total)
            total = total + sums[:, LANES:]
        return jnp.concatenate(out, axis=1), total

    rank, total = ranked(chosen, jnp.zeros((8, LANES), F32))
    stay_to = jnp.where(chosen[0:1] > 0.5, rank[0:1], -1.0).astype(I32)
    slot_to = rank + (half * (sub - 1)).astype(F32)
    leaving = (sub >= 1) & (chosen > 0.5)
    leave_to = (jnp.sum(jnp.where(leaving, slot_to + 1.0, 0.0), axis=0, keepdims=True) - 1.0).astype(I32)
    position = jnp.zeros((8, wide), F32)
    for n in range(3):
        position = jnp.where(sub == n, off_ref[n, :, 0:wide], position)
    marks = jnp.where(sub == 0, i_row, jnp.where(sub == 1, j_row, jnp.where(sub == 2, k_row, 1)))
    raw = lax.dot_general(
        jnp.concatenate([thirds(position).astype(F32), marks.astype(F32)], axis=0).astype(BF16),
        slots_of(leave_to, few), NT, preferred_element_type=F32,
    )
    first_position = raw[0:8] + raw[8:16] + raw[16:24]
    first_i, first_j, first_k = (
        jnp.clip(raw[24 + n : 25 + n].astype(I32), 0, top_value)
        for n, top_value in enumerate((cols - 1, rows - 1, depth - 2))
    )
    first_real = raw[27:28] > 0.5

    def words(i, j, k, target):
        start = jnp.where(i >= LANES, span, 0) + k * level + 4 * j
        start = start * LANES + ((iota(i.shape, 1) - i) & (LANES - 1))
        for t in range(i.shape[1] // LANES):
            part = start[:, t * LANES : (t + 1) * LANES]
            target[2 * t : 2 * t + 1, :] = part
            target[2 * t + 1 : 2 * t + 2, :] = pltpu.roll(part, half, 1)

    words(first_i, first_j, first_k, first_ref)
    words(i_row, j_row, k_row, where_ref)
    addresses = [
        pltpu.make_async_copy(first_ref, first_smem, asem.at[0]),
        pltpu.make_async_copy(where_ref, where_smem, asem.at[1]),
    ]
    for copy in addresses:
        copy.start()
    stay_ref[...] = slots_of(stay_to, wide)

    for part in range(2):
        table[pl.ds(part * span + depth * level, span - depth * level), :] = jnp.zeros(
            (span - depth * level, LANES), F32
        )
    side[...] = jnp.zeros_like(side)
    gathered[...] = jnp.zeros_like(gathered)
    first_gathered[...] = jnp.zeros_like(first_gathered)
    first_lane = jnp.where(lane == 0, 1.0, 0.0).astype(BF16)
    for c in range(3):
        loads[c].wait()

        def build(step, carry):
            for u in range(5):
                k = step * 5 + u
                for h in range(2):
                    plane = vel[c, k, :, h * LANES : (h + 1) * LANES].astype(F32)
                    for s in range(rows // 8):
                        at = h * span + k * level + 32 * s + c
                        table[pl.ds(at, 8, stride=4), :] = plane[8 * s : 8 * s + 8]
            return carry

        lax.fori_loop(0, depth // 5, build, 0)

        for h in range(2):
            plane = vel[c, :, :, h * LANES : (h + 1) * LANES].reshape(depth * rows, LANES)
            line = lax.dot_general(first_lane, plane, NT, preferred_element_type=F32)[0:1]
            for g in range(pl.cdiv(depth, per)):
                n = min(LANES, depth * rows - g * LANES)
                side[h * 3 + c, g : g + 1, 0:n] = line[:, g * LANES : g * LANES + n]
    column[...] = side[0:3].astype(BF16)

    def edge(target, ends, row):
        firsts = [jnp.zeros((8, deep), F32)] * 2
        for h in range(2):
            for c in range(3):
                blocks = []
                for block in range(deep // 8):
                    at = h * span + block * 8 * level + 4 * row + c
                    blocks.append(table[pl.ds(at, 8, stride=level), :])
                plane = jnp.concatenate(blocks, axis=0).astype(BF16)
                target[pl.ds(h * deep, deep), pl.ds(c * LANES, LANES)] = plane
                pick = jnp.where((lane == 0) & (iota((8, LANES), 0) == c), 1.0, 0.0).astype(BF16)
                firsts[h] = firsts[h] + lax.dot_general(pick, plane, NT, preferred_element_type=F32)
        pad = jnp.zeros((8, LANES - deep), F32)
        tail = jnp.concatenate([jnp.concatenate([firsts[1], pad], axis=1), jnp.zeros((8, LANES), F32)], axis=0)
        target[2 * deep : 2 * deep + 16, :] = jnp.concatenate([tail, jnp.zeros((16, 2 * LANES), F32)], axis=1).astype(BF16)
        ends[...] = jnp.concatenate([firsts[0], pad], axis=1)

    edge(nrow, cnr, 0)

    @pl.when(top)
    def _():
        edge(nfold, cfold, rows - 1)

    def remote(src, dst, s, t, lat, lon):
        return pltpu.make_async_remote_copy(
            src, dst, send.at[s], recv.at[t], device_id=(lon, lat), device_id_type=MESH
        )

    col_out = remote(column, col_in, 0, 0, r, west)
    row_out = remote(nrow, nrow_in, 1, 1, r - 1, p)
    cnr_out = remote(cnr, cnr_in, 2, 2, r - 1, west)
    fold_out = remote(nfold, nrow_in, 3, 1, r, across)
    cfold_out = remote(cfold, cnr_in, 4, 2, r, corner)
    cfold_here = pltpu.make_async_copy(cfold, cnr_in, lsem)

    peers = 2 + 2 * (r > 0).astype(I32) + (r < n_lat - 1).astype(I32) + top.astype(I32) + away.astype(I32)
    pl.semaphore_wait(barrier, peers)

    @pl.when(r > 0)
    def _():
        row_out.start()
        cnr_out.start()

    @pl.when(top)
    def _():
        fold_out.start()

    @pl.when(away)
    def _():
        cfold_out.start()

    @pl.when(jnp.logical_and(top, corner == p))
    def _():
        cfold_here.start()

    col_out.start()

    def gather(source, target, count):
        def body(step, carry):
            base = (step & 1) * half
            group = step >> 1
            ahead = lane - base
            accs = [target[n, group] for n in range(4)]
            for u in range(count):
                word = source[step, u]
                at, shift = word >> 7, word & (LANES - 1)
                here = ahead == u
                there = ahead == u + 1 if u < half - 1 else lane == ((base + half) & (LANES - 1))
                for dk in range(2):
                    turned = pltpu.roll(table[pl.ds(at + dk * level, 8), :], shift, 1)
                    accs[2 * dk] = jnp.where(here, turned, accs[2 * dk])
                    accs[2 * dk + 1] = jnp.where(there, turned, accs[2 * dk + 1])
            for n in range(4):
                target[n, group] = accs[n]
            return carry

        return body

    def together(source, w):
        out = []
        for dk in range(2):
            low = [source[2 * dk, t] for t in range(w // LANES)]
            high = [pltpu.roll(source[2 * dk + 1, t], LANES - 1, 1) for t in range(w // LANES)]
            out.append([jnp.concatenate(low, axis=1), jnp.concatenate(high, axis=1)])
        return out

    addresses[0].wait()
    lax.fori_loop(0, 4, gather(first_smem, first_gathered, CAP), 0)
    addresses[1].wait()

    go = iota((1, few), 1) // half + 1
    folding = (go == 3) & top
    last_i, last_j = cols - 1, rows - 1
    new_i = jnp.where(
        go == 1, 0, jnp.where(go == 2, last_i, jnp.where(folding, last_i - first_i, first_i))
    )
    new_j = jnp.where(
        go == 3, jnp.where(top, last_j, 0), jnp.where(go == 4, last_j, first_j)
    )
    code = jnp.where(first_real, 1 + new_i + cols * (new_j + rows * first_k), 0).astype(F32)

    cnr_wait = remote(cnr, cnr_in, 2, 2, r, west)
    col_out.wait_recv()
    row_out.wait_recv()

    @pl.when(jnp.logical_or(jnp.logical_not(top), corner != p))
    def _():
        cnr_wait.wait_recv()

    @pl.when(jnp.logical_and(top, corner == p))
    def _():
        cfold_here.wait()

    sides = []
    for c in range(3):
        lines = jnp.concatenate([side[3 + c], col_in[c].astype(F32)], axis=0)
        lines = [lines if m == 0 else pltpu.roll(lines, LANES - m * rows, 1) for m in range(per)]
        sides.append(jnp.concatenate(lines, axis=0).T[0:rows].astype(BF16))

    corners = halo_corners(
        few, first_i, first_j, first_k, together(first_gathered, few), top, sides, nrow_in, cnr_in
    )
    moved = advanced(corners, first_position)
    na, nb, nc = moved[0:1], moved[1:2], moved[2:3]
    new_a = jnp.where(go == 1, na - 1.0, jnp.where(go == 2, na + 1.0, jnp.where(folding, 1.0 - na, na)))
    new_b = jnp.where(go == 3, jnp.where(top, 2.0 - nb, nb - 1.0), jnp.where(go == 4, nb + 1.0, nb))
    sub_few = iota((8, few), 0)
    records = jnp.where(
        sub_few == 0, new_a,
        jnp.where(sub_few == 1, new_b, jnp.where(sub_few == 2, nc, jnp.where(sub_few == 3, code, 0.0))),
    )
    records = jnp.where(first_real, records, 0.0)

    for m in range(2):
        pack[m] = records[:, m * LANES : (m + 1) * LANES]

    @pl.when(r == 0)
    def _():
        pack_in[2] = jnp.zeros((8, LANES), F32)

    east_out = remote(pack.at[0], pack_in.at[0], 5, 3, r, east)
    west_out = remote(pack.at[0], pack_in.at[1], 6, 4, r, west)
    north_out = remote(pack.at[1], pack_in.at[2], 7, 5, r + 1, p)
    over_out = remote(pack.at[1], pack_in.at[3], 7, 6, r, across)
    south_out = remote(pack.at[1], pack_in.at[3], 8, 6, r - 1, p)

    @pl.when(top)
    def _():
        over_out.start()

    @pl.when(r < n_lat - 1)
    def _():
        north_out.start()

    @pl.when(r > 0)
    def _():
        south_out.start()

    east_out.start()
    west_out.start()

    lax.fori_loop(0, live // half, gather(where_smem, gathered, half), 0)
    corners = halo_corners(
        wide, i_row, j_row, k_row, together(gathered, wide), top, sides, nrow_in, cnr_in
    )
    moved = advanced(corners, position)
    code = (1 + i_row + cols * (j_row + rows * k_row)).astype(F32)
    kept = placed(jnp.where(sub < 3, moved, jnp.where(sub == 3, code, 0.0)), stay_ref[...])

    east_out.wait_recv()
    west_out.wait_recv()

    @pl.when(r > 0)
    def _():
        north_out.wait_recv()

    over_out.wait_recv()

    from_north = jnp.where(top, pltpu.roll(pack_in[3], half, 1), pack_in[3])
    arrivals = jnp.concatenate(
        [
            jnp.where(lane < half, pack_in[0], pack_in[1]),
            jnp.where(lane < half, pack_in[2], from_north),
        ],
        axis=1,
    )
    present = jnp.where(arrivals > 0.5, 1.0, 0.0)
    order, filled = ranked(present, jnp.broadcast_to(total[0:1], (8, LANES)))
    arrive_to = jnp.where(present[3:4] > 0.5, order[3:4], -1.0).astype(I32)
    joined = placed(arrivals, slots_of(arrive_to, slots))
    result = joined + jnp.concatenate([kept, jnp.zeros((8, slots - wide), F32)], axis=1)
    out_ref[...] = jnp.where(iota((8, slots), 0) == 4, filled[3:4, 0:1], result)

    col_out.wait_send()
    east_out.wait_send()
    west_out.wait_send()
    north_out.wait_send()

    @pl.when(r > 0)
    def _():
        row_out.wait_send()
        cnr_out.wait_send()
        south_out.wait_send()

    @pl.when(top)
    def _():
        fold_out.wait_send()

    @pl.when(away)
    def _():
        cfold_out.wait_send()


def decode(rows, cols, result_ref, new_off, new_cell, new_count):
    for n in range(3):
        new_off[n] = result_ref[n : n + 1, :]
    code = jnp.maximum(result_ref[3:4, :].astype(I32) - 1, 0)
    new_cell[0] = code & (cols - 1)
    new_cell[1] = (code // cols) & (rows - 1)
    new_cell[2] = code // (cols * rows)
    new_count[...] = result_ref[4:5, 0:1].astype(I32)


def shards(velocity, offsets, cells, counts, moves):
    _, depth, rows, cols = velocity.shape
    slots = offsets.shape[2]
    live = slots * 3 // 4
    wide = pl.cdiv(live, LANES) * LANES
    deep = pl.cdiv(depth, 16) * 16
    dims = (depth, rows, cols, slots, live, lax.axis_size("lat"), lax.axis_size("lon"))
    groups = pl.cdiv(depth * rows, 8 * LANES) * 8
    vmem = pl.BlockSpec(memory_space=pltpu.VMEM)
    hbm = pl.BlockSpec(memory_space=pltpu.HBM)
    velocity, offsets, cells, moves = (
        pltpu.with_memory_space_constraint(x, pltpu.HBM) for x in (velocity, offsets, cells, moves)
    )
    result = pl.pallas_call(
        functools.partial(kernel, dims),
        out_shape=jax.ShapeDtypeStruct((8, slots), F32),
        in_specs=[hbm] * 5,
        out_specs=vmem,
        scratch_shapes=[
            pltpu.VMEM((3, depth, rows, cols), BF16),
            pltpu.VMEM((3, 1, slots), F32),
            pltpu.VMEM((3, 1, slots), I32),
            pltpu.VMEM((1, slots), I32),
            pltpu.VMEM((1, 1), I32),
            pltpu.VMEM((2 * deep * rows * 4, LANES), F32),
            pltpu.VMEM((2 * wide // LANES, LANES), I32),
            pltpu.SMEM((2 * wide // LANES, LANES), I32),
            pltpu.VMEM((4, LANES), I32),
            pltpu.SMEM((4, LANES), I32),
            pltpu.VMEM((4, wide // LANES, 8, LANES), F32),
            pltpu.VMEM((4, 2, 8, LANES), F32),
            pltpu.VMEM((wide, wide), BF16),
            pltpu.VMEM((6, groups, LANES), F32),
            pltpu.VMEM((3, groups, LANES), BF16),
            pltpu.VMEM((2 * deep + 16, 3 * LANES), BF16),
            pltpu.VMEM((2 * deep + 16, 3 * LANES), BF16),
            pltpu.VMEM((8, LANES), F32),
            pltpu.VMEM((8, LANES), F32),
            pltpu.VMEM((3, groups, LANES), BF16),
            pltpu.VMEM((2 * deep + 16, 3 * LANES), BF16),
            pltpu.VMEM((8, LANES), F32),
            pltpu.VMEM((2, 8, LANES), F32),
            pltpu.VMEM((4, 8, LANES), F32),
            pltpu.SemaphoreType.DMA((3,)),
            pltpu.SemaphoreType.DMA((4,)),
            pltpu.SemaphoreType.DMA((9,)),
            pltpu.SemaphoreType.DMA((7,)),
            pltpu.SemaphoreType.DMA,
            pltpu.SemaphoreType.DMA((2,)),
        ],
        compiler_params=pltpu.CompilerParams(
            collective_id=0, has_side_effects=True, vmem_limit_bytes=32 * 1024 * 1024
        ),
        name="advance",
    )(velocity, offsets, cells, counts, moves)
    return pl.pallas_call(
        functools.partial(decode, rows, cols),
        out_shape=(
            jax.ShapeDtypeStruct((3, 1, slots), F32),
            jax.ShapeDtypeStruct((3, 1, slots), I32),
            jax.ShapeDtypeStruct((1, 1), I32),
        ),
        in_specs=[vmem],
        out_specs=(vmem, vmem, vmem),
        compiler_params=pltpu.CompilerParams(vmem_limit_bytes=1024 * 1024),
        name="decode",
    )(result)


def solution(mesh):
    placed_in = (
        P(None, None, "lat", "lon"),
        P(None, "lat", "lon"),
        P(None, "lat", "lon"),
        P("lat", "lon"),
        P("lat", "lon"),
    )
    return jax.shard_map(
        shards,
        mesh=mesh,
        in_specs=placed_in,
        out_specs=(P(None, "lat", "lon"), P(None, "lat", "lon"), P("lat", "lon")),
        check_vma=False,
    )
```

```python
import functools

import jax
import jax.numpy as jnp
from jax import lax
from jax.experimental import pallas as pl
from jax.experimental.pallas import tpu as pltpu
from jax.sharding import PartitionSpec as P

MESH = pl.DeviceIdType.MESH
CAP = 48
LANES = 128
F32, BF16, I32 = jnp.float32, jnp.bfloat16, jnp.int32
NT = (((1,), (1,)), ((), ()))
TN = (((0,), (0,)), ((), ()))


def iota(shape, dim):
    return lax.broadcasted_iota(I32, shape, dim)


def thirds(x):
    high = x.astype(BF16)
    rest = x - high.astype(F32)
    mid = rest.astype(BF16)
    low = (rest - mid.astype(F32)).astype(BF16)
    return jnp.concatenate([high.astype(F32), mid.astype(F32), low.astype(F32)], axis=0).astype(BF16)


def slots_of(target, size):
    return jnp.where(iota((size, target.shape[1]), 0) == target, 1.0, 0.0).astype(BF16)


def placed(records, onehot):
    out = lax.dot_general(thirds(records), onehot, NT, preferred_element_type=F32)
    return out[0:8] + out[8:16] + out[16:24]


def velocity_at(corners, a_row, b_row, c_row):
    sub = iota((8, a_row.shape[1]), 0)
    wb = jnp.where(sub < 4, 1.0 - b_row, b_row)
    w0 = (wb * (1.0 - c_row)).astype(BF16).astype(F32)
    w1 = (wb * c_row).astype(BF16).astype(F32)
    sums = []
    for d in range(2):
        s = w0 * corners[0][d] + w1 * corners[1][d]
        sums.append(s + pltpu.roll(s, 4, 0))
    return (1.0 - a_row) * sums[0] + a_row * sums[1]


def halo_corners(w, i_row, j_row, k_row, inside, top, sides, nrow_in, cnr_in):
    cols, rows = 2 * LANES, sides[0].shape[0]
    deep = (nrow_in.shape[0] - 16) // 2
    groups = sides[0].shape[1] // 8
    per = LANES // rows
    sub2 = iota((8, 2 * w), 0)

    def twice(x):
        return jnp.concatenate([x] * 2, axis=1)

    def hot(size, at):
        return jnp.where(iota((size, 2 * w), 0) == at, 1.0, 0.0).astype(BF16)

    k2 = jnp.concatenate([k_row, k_row + 1], axis=1)
    j2 = twice(j_row)
    outer = twice(jnp.where(i_row == cols - 1, groups, 0))
    at_side = hot(8 * groups, (k2 & (per - 1)) * (2 * groups) + outer + lax.shift_right_logical(k2, per.bit_length() - 1))
    base = twice(jnp.where(top, cols - 1 - i_row, i_row))
    second = base >= LANES
    inner = base & (LANES - 1)
    at_row = hot(2 * deep, k2 + jnp.where(second, deep, 0))
    at_level = hot(LANES, k2)

    eastern = jnp.zeros((8, 2 * w), F32)
    hits = [iota((rows, 2 * w), 0) == j2 + dj for dj in range(2)]
    for c in range(3):
        found = jnp.dot(sides[c], at_side, preferred_element_type=F32)
        for dj in range(2):
            value = jnp.sum(jnp.where(hits[dj], found, 0.0), axis=0, keepdims=True)
            eastern = jnp.where(sub2 == 4 * dj + c, value, eastern)

    few = jnp.concatenate([cnr_in[...], nrow_in[2 * deep :, 0:LANES].astype(F32)], axis=0).astype(BF16)
    ends = jnp.dot(few, at_level, preferred_element_type=F32)
    last = pltpu.roll(jnp.where(second, ends[0:8], ends[8:16]), 4, 0)

    pair = [jnp.zeros((8, 2 * w), F32), last]
    lane_id = iota((LANES, 2 * w), 0)
    hits = [lane_id == inner, lane_id == inner + 1]
    for c in range(3):
        found = lax.dot_general(
            nrow_in[0 : 2 * deep, c * LANES : (c + 1) * LANES], at_row, TN, preferred_element_type=F32
        )
        for d in range(2):
            value = jnp.sum(jnp.where(hits[d], found, 0.0), axis=0, keepdims=True)
            put = sub2 == 4 + c
            pair[d] = jnp.where(put & (inner < LANES - 1) if d else put, value, pair[d])

    sign = jnp.where(top, -1.0, 1.0)
    north = [sign * jnp.where(top, pair[1 - d], pair[d]) for d in range(2)]
    lower = iota((8, w), 0) >= 4
    corners = []
    for dk in range(2):
        part = slice(dk * w, (dk + 1) * w)
        out = []
        for d in range(2):
            here = inside[dk][d]
            if d == 1:
                here = jnp.where((i_row & (LANES - 1)) == LANES - 1, eastern[:, part], here)
            out.append(jnp.where(lower & (j_row == rows - 1), north[d][:, part], here))
        corners.append(out)
    return corners


def advanced(corners, position):
    first = velocity_at(corners, position[0:1], position[1:2], position[2:3])
    middle = position + 0.5 * first
    return position + velocity_at(corners, middle[0:1], middle[1:2], middle[2:3])


def kernel(
    dims, vel_hbm, off_hbm, cell_hbm, count_hbm, move_hbm,
    out_ref,
    vel, off_ref, cell_ref, move_ref, count_ref, table, where_ref, where_smem, first_ref, first_smem,
    gathered, first_gathered, stay_ref,
    side, column, nrow, nfold, cnr, cfold, col_in, nrow_in, cnr_in,
    pack, pack_in, vsem, isem, send, recv, lsem, asem,
):
    depth, rows, cols, slots, live, n_lat, n_lon = dims
    wide = pl.cdiv(live, LANES) * LANES
    tiles = wide // LANES
    half = LANES // 2
    few = 4 * half
    level = rows * 4
    span = table.shape[0] // 2
    deep = span // level
    per = LANES // rows
    groups = side.shape[1]
    r, p = lax.axis_index("lat"), lax.axis_index("lon")
    east, west = lax.rem(p + 1, n_lon), lax.rem(p + n_lon - 1, n_lon)
    across, corner = n_lon - 1 - p, lax.rem(n_lon - p, n_lon)
    top = r == n_lat - 1
    away = jnp.logical_and(top, corner != p)

    smalls = [(cell_hbm, cell_ref), (move_hbm, move_ref), (count_hbm, count_ref), (off_hbm, off_ref)]
    smalls = [pltpu.make_async_copy(src, dst, isem.at[n]) for n, (src, dst) in enumerate(smalls)]
    for small in smalls:
        small.start()
    bands = [slice(8 * n, 8 * n + 8) for n in range(rows // 8)]
    bands = [bands[0], bands[-1]] + bands[1:-1]
    loads = [
        pltpu.make_async_copy(vel_hbm.at[:, :, band, :], vel.at[:, :, band, :], vsem.at[n])
        for n, band in enumerate(bands)
    ]
    for load in loads:
        load.start()

    barrier = pltpu.get_barrier_semaphore()

    def greet(lat, lon):
        pl.semaphore_signal(barrier, inc=1, device_id=(lon, lat), device_id_type=MESH)

    greet(r, east)
    greet(r, west)

    @pl.when(r < n_lat - 1)
    def _():
        greet(r + 1, p)
        greet(r + 1, east)

    @pl.when(r > 0)
    def _():
        greet(r - 1, p)

    @pl.when(top)
    def _():
        greet(r, across)

    @pl.when(away)
    def _():
        greet(r, corner)

    lane = iota((8, LANES), 1)
    sub = iota((8, wide), 0)
    for small in smalls:
        small.wait()

    i_row, j_row, k_row = (cell_ref[n, :, 0:wide] for n in range(3))
    motion = move_ref[:, 0:wide]
    valid = iota((1, wide), 1) < count_ref[...]
    chosen = jnp.where((sub == motion) & valid, 1.0, 0.0)
    before = jnp.where(iota((LANES, LANES), 0) < iota((LANES, LANES), 1), 1.0, 0.0).astype(BF16)
    upto = jnp.concatenate([before, jnp.ones((LANES, LANES), BF16)], axis=1)

    def ranked(flags, total):
        out = []
        for t in range(flags.shape[1] // LANES):
            sums = jnp.dot(
                flags[:, t * LANES : (t + 1) * LANES].astype(BF16), upto, preferred_element_type=F32
            )
            out.append(sums[:, :LANES] + total)
            total = total + sums[:, LANES:]
        return jnp.concatenate(out, axis=1), total

    rank, total = ranked(chosen, jnp.zeros((8, LANES), F32))
    stay_to = jnp.where(chosen[0:1] > 0.5, rank[0:1], -1.0).astype(I32)
    slot_to = rank + (half * (sub - 1)).astype(F32)
    leaving = (sub >= 1) & (chosen > 0.5)
    leave_to = (jnp.sum(jnp.where(leaving, slot_to + 1.0, 0.0), axis=0, keepdims=True) - 1.0).astype(I32)
    position = jnp.zeros((8, wide), F32)
    for n in range(3):
        position = jnp.where(sub == n, off_ref[n, :, 0:wide], position)
    marks = jnp.where(sub == 0, i_row, jnp.where(sub == 1, j_row, jnp.where(sub == 2, k_row, 1)))
    raw = lax.dot_general(
        jnp.concatenate([thirds(position).astype(F32), marks.astype(F32)], axis=0).astype(BF16),
        slots_of(leave_to, few), NT, preferred_element_type=F32,
    )
    first_position = raw[0:8] + raw[8:16] + raw[16:24]
    first_i, first_j, first_k = (
        jnp.clip(raw[24 + n : 25 + n].astype(I32), 0, top_value)
        for n, top_value in enumerate((cols - 1, rows - 1, depth - 2))
    )
    first_real = raw[27:28] > 0.5

    def words(i, j, k, target):
        start = jnp.where(i >= LANES, span, 0) + k * level + 4 * j
        start = start * LANES + ((iota(i.shape, 1) - i) & (LANES - 1))
        for t in range(i.shape[1] // LANES):
            part = start[:, t * LANES : (t + 1) * LANES]
            target[2 * t : 2 * t + 1, :] = part
            target[2 * t + 1 : 2 * t + 2, :] = pltpu.roll(part, half, 1)

    words(first_i, first_j, first_k, first_ref)
    words(i_row, j_row, k_row, where_ref)
    addresses = [
        pltpu.make_async_copy(first_ref, first_smem, asem.at[0]),
        pltpu.make_async_copy(where_ref, where_smem, asem.at[1]),
    ]
    for copy in addresses:
        copy.start()
    stay_ref[...] = slots_of(stay_to, wide)

    for part in range(2):
        table[pl.ds(part * span + depth * level, span - depth * level), :] = jnp.zeros(
            (span - depth * level, LANES), F32
        )
    side[...] = jnp.zeros_like(side)
    gathered[...] = jnp.zeros_like(gathered)
    first_gathered[...] = jnp.zeros_like(first_gathered)
    first_lane = jnp.where(lane == 0, 1.0, 0.0).astype(BF16)

    def build(n):
        band = bands[n]
        loads[n].wait()

        def body(step, carry):
            for u in range(5):
                k = step * 5 + u
                for c in range(3):
                    for h in range(2):
                        at = h * span + k * level + 4 * band.start + c
                        table[pl.ds(at, 8, stride=4), :] = vel[c, k, band, h * LANES : (h + 1) * LANES].astype(F32)
            return carry

        lax.fori_loop(0, depth // 5, body, 0)

    def edge(target, ends, row):
        firsts = [jnp.zeros((8, deep), F32)] * 2
        for h in range(2):
            for c in range(3):
                blocks = []
                for block in range(deep // 8):
                    at = h * span + block * 8 * level + 4 * row + c
                    blocks.append(table[pl.ds(at, 8, stride=level), :])
                plane = jnp.concatenate(blocks, axis=0).astype(BF16)
                target[pl.ds(h * deep, deep), pl.ds(c * LANES, LANES)] = plane
                pick = jnp.where((lane == 0) & (iota((8, LANES), 0) == c), 1.0, 0.0).astype(BF16)
                firsts[h] = firsts[h] + lax.dot_general(pick, plane, NT, preferred_element_type=F32)
        pad = jnp.zeros((8, LANES - deep), F32)
        tail = jnp.concatenate([jnp.concatenate([firsts[1], pad], axis=1), jnp.zeros((8, LANES), F32)], axis=0)
        target[2 * deep : 2 * deep + 16, :] = jnp.concatenate([tail, jnp.zeros((16, 2 * LANES), F32)], axis=1).astype(BF16)
        ends[...] = jnp.concatenate([firsts[0], pad], axis=1)

    def remote(src, dst, s, t, lat, lon):
        return pltpu.make_async_remote_copy(
            src, dst, send.at[s], recv.at[t], device_id=(lon, lat), device_id_type=MESH
        )

    col_out = remote(column, col_in, 0, 0, r, west)
    row_out = remote(nrow, nrow_in, 1, 1, r - 1, p)
    cnr_out = remote(cnr, cnr_in, 2, 2, r - 1, west)
    fold_out = remote(nfold, nrow_in, 3, 1, r, across)
    cfold_out = remote(cfold, cnr_in, 4, 2, r, corner)
    cfold_here = pltpu.make_async_copy(cfold, cnr_in, lsem)

    build(0)
    edge(nrow, cnr, 0)
    peers = 2 + 2 * (r > 0).astype(I32) + (r < n_lat - 1).astype(I32) + top.astype(I32) + away.astype(I32)
    pl.semaphore_wait(barrier, peers)

    @pl.when(r > 0)
    def _():
        row_out.start()
        cnr_out.start()

    build(1)

    @pl.when(top)
    def _():
        edge(nfold, cfold, rows - 1)
        fold_out.start()

    @pl.when(away)
    def _():
        cfold_out.start()

    @pl.when(jnp.logical_and(top, corner == p))
    def _():
        cfold_here.start()

    for n in range(2, len(bands)):
        build(n)

    for c in range(3):
        for h in range(2):
            plane = vel[c, :, :, h * LANES : (h + 1) * LANES].reshape(depth * rows, LANES)
            line = lax.dot_general(first_lane, plane, NT, preferred_element_type=F32)[0:1]
            for g in range(pl.cdiv(depth, per)):
                n = min(LANES, depth * rows - g * LANES)
                side[h * 3 + c, g : g + 1, 0:n] = line[:, g * LANES : g * LANES + n]
    column[...] = side[0:3].astype(BF16)
    col_out.start()

    def gather(source, target, count):
        def body(step, carry):
            base = (step & 1) * half
            group = step >> 1
            ahead = lane - base
            accs = [target[n, group] for n in range(4)]
            for u in range(count):
                word = source[step, u]
                at, shift = word >> 7, word & (LANES - 1)
                here = ahead == u
                there = ahead == u + 1 if u < half - 1 else lane == ((base + half) & (LANES - 1))
                for dk in range(2):
                    turned = pltpu.roll(table[pl.ds(at + dk * level, 8), :], shift, 1)
                    accs[2 * dk] = jnp.where(here, turned, accs[2 * dk])
                    accs[2 * dk + 1] = jnp.where(there, turned, accs[2 * dk + 1])
            for n in range(4):
                target[n, group] = accs[n]
            return carry

        return body

    def together(source, w):
        out = []
        for dk in range(2):
            low = [source[2 * dk, t] for t in range(w // LANES)]
            high = [pltpu.roll(source[2 * dk + 1, t], LANES - 1, 1) for t in range(w // LANES)]
            out.append([jnp.concatenate(low, axis=1), jnp.concatenate(high, axis=1)])
        return out

    for copy in addresses:
        copy.wait()
    lax.fori_loop(0, 4, gather(first_smem, first_gathered, CAP), 0)
    lax.fori_loop(0, live // half, gather(where_smem, gathered, half), 0)

    go = iota((1, few), 1) // half + 1
    folding = (go == 3) & top
    last_i, last_j = cols - 1, rows - 1
    new_i = jnp.where(
        go == 1, 0, jnp.where(go == 2, last_i, jnp.where(folding, last_i - first_i, first_i))
    )
    new_j = jnp.where(
        go == 3, jnp.where(top, last_j, 0), jnp.where(go == 4, last_j, first_j)
    )
    code = jnp.where(first_real, 1 + new_i + cols * (new_j + rows * first_k), 0).astype(F32)

    cnr_wait = remote(cnr, cnr_in, 2, 2, r, west)
    col_out.wait_recv()
    row_out.wait_recv()

    @pl.when(jnp.logical_or(jnp.logical_not(top), corner != p))
    def _():
        cnr_wait.wait_recv()

    @pl.when(jnp.logical_and(top, corner == p))
    def _():
        cfold_here.wait()

    sides = []
    for c in range(3):
        lines = jnp.concatenate([side[3 + c], col_in[c].astype(F32)], axis=0)
        lines = [lines if m == 0 else pltpu.roll(lines, LANES - m * rows, 1) for m in range(per)]
        sides.append(jnp.concatenate(lines, axis=0).T[0:rows].astype(BF16))

    corners = halo_corners(
        few, first_i, first_j, first_k, together(first_gathered, few), top, sides, nrow_in, cnr_in
    )
    moved = advanced(corners, first_position)
    na, nb, nc = moved[0:1], moved[1:2], moved[2:3]
    new_a = jnp.where(go == 1, na - 1.0, jnp.where(go == 2, na + 1.0, jnp.where(folding, 1.0 - na, na)))
    new_b = jnp.where(go == 3, jnp.where(top, 2.0 - nb, nb - 1.0), jnp.where(go == 4, nb + 1.0, nb))
    sub_few = iota((8, few), 0)
    records = jnp.where(
        sub_few == 0, new_a,
        jnp.where(sub_few == 1, new_b, jnp.where(sub_few == 2, nc, jnp.where(sub_few == 3, code, 0.0))),
    )
    records = jnp.where(first_real, records, 0.0)

    for m in range(2):
        pack[m] = records[:, m * LANES : (m + 1) * LANES]

    @pl.when(r == 0)
    def _():
        pack_in[2] = jnp.zeros((8, LANES), F32)

    east_out = remote(pack.at[0], pack_in.at[0], 5, 3, r, east)
    west_out = remote(pack.at[0], pack_in.at[1], 6, 4, r, west)
    north_out = remote(pack.at[1], pack_in.at[2], 7, 5, r + 1, p)
    over_out = remote(pack.at[1], pack_in.at[3], 7, 6, r, across)
    south_out = remote(pack.at[1], pack_in.at[3], 8, 6, r - 1, p)

    @pl.when(top)
    def _():
        over_out.start()

    @pl.when(r < n_lat - 1)
    def _():
        north_out.start()

    @pl.when(r > 0)
    def _():
        south_out.start()

    east_out.start()
    west_out.start()

    corners = halo_corners(
        wide, i_row, j_row, k_row, together(gathered, wide), top, sides, nrow_in, cnr_in
    )
    moved = advanced(corners, position)
    code = (1 + i_row + cols * (j_row + rows * k_row)).astype(F32)
    kept = placed(jnp.where(sub < 3, moved, jnp.where(sub == 3, code, 0.0)), stay_ref[...])

    east_out.wait_recv()
    west_out.wait_recv()

    @pl.when(r > 0)
    def _():
        north_out.wait_recv()

    over_out.wait_recv()

    from_north = jnp.where(top, pltpu.roll(pack_in[3], half, 1), pack_in[3])
    arrivals = jnp.concatenate(
        [
            jnp.where(lane < half, pack_in[0], pack_in[1]),
            jnp.where(lane < half, pack_in[2], from_north),
        ],
        axis=1,
    )
    present = jnp.where(arrivals > 0.5, 1.0, 0.0)
    order, filled = ranked(present, jnp.broadcast_to(total[0:1], (8, LANES)))
    arrive_to = jnp.where(present[3:4] > 0.5, order[3:4], -1.0).astype(I32)
    joined = placed(arrivals, slots_of(arrive_to, slots))
    result = joined + jnp.concatenate([kept, jnp.zeros((8, slots - wide), F32)], axis=1)
    out_ref[...] = jnp.where(iota((8, slots), 0) == 4, filled[3:4, 0:1], result)

    col_out.wait_send()
    east_out.wait_send()
    west_out.wait_send()
    north_out.wait_send()

    @pl.when(r > 0)
    def _():
        row_out.wait_send()
        cnr_out.wait_send()
        south_out.wait_send()

    @pl.when(top)
    def _():
        fold_out.wait_send()

    @pl.when(away)
    def _():
        cfold_out.wait_send()


def decode(rows, cols, result_ref, new_off, new_cell, new_count):
    for n in range(3):
        new_off[n] = result_ref[n : n + 1, :]
    code = jnp.maximum(result_ref[3:4, :].astype(I32) - 1, 0)
    new_cell[0] = code & (cols - 1)
    new_cell[1] = (code // cols) & (rows - 1)
    new_cell[2] = code // (cols * rows)
    new_count[...] = result_ref[4:5, 0:1].astype(I32)


def shards(velocity, offsets, cells, counts, moves):
    _, depth, rows, cols = velocity.shape
    slots = offsets.shape[2]
    live = slots * 3 // 4
    wide = pl.cdiv(live, LANES) * LANES
    deep = pl.cdiv(depth, 16) * 16
    dims = (depth, rows, cols, slots, live, lax.axis_size("lat"), lax.axis_size("lon"))
    groups = pl.cdiv(depth * rows, 8 * LANES) * 8
    vmem = pl.BlockSpec(memory_space=pltpu.VMEM)
    hbm = pl.BlockSpec(memory_space=pltpu.HBM)
    velocity, offsets, cells, moves = (
        pltpu.with_memory_space_constraint(x, pltpu.HBM) for x in (velocity, offsets, cells, moves)
    )
    result = pl.pallas_call(
        functools.partial(kernel, dims),
        out_shape=jax.ShapeDtypeStruct((8, slots), F32),
        in_specs=[hbm] * 5,
        out_specs=vmem,
        scratch_shapes=[
            pltpu.VMEM((3, depth, rows, cols), BF16),
            pltpu.VMEM((3, 1, slots), F32),
            pltpu.VMEM((3, 1, slots), I32),
            pltpu.VMEM((1, slots), I32),
            pltpu.VMEM((1, 1), I32),
            pltpu.VMEM((2 * deep * rows * 4, LANES), F32),
            pltpu.VMEM((2 * wide // LANES, LANES), I32),
            pltpu.SMEM((2 * wide // LANES, LANES), I32),
            pltpu.VMEM((4, LANES), I32),
            pltpu.SMEM((4, LANES), I32),
            pltpu.VMEM((4, wide // LANES, 8, LANES), F32),
            pltpu.VMEM((4, 2, 8, LANES), F32),
            pltpu.VMEM((wide, wide), BF16),
            pltpu.VMEM((6, groups, LANES), F32),
            pltpu.VMEM((3, groups, LANES), BF16),
            pltpu.VMEM((2 * deep + 16, 3 * LANES), BF16),
            pltpu.VMEM((2 * deep + 16, 3 * LANES), BF16),
            pltpu.VMEM((8, LANES), F32),
            pltpu.VMEM((8, LANES), F32),
            pltpu.VMEM((3, groups, LANES), BF16),
            pltpu.VMEM((2 * deep + 16, 3 * LANES), BF16),
            pltpu.VMEM((8, LANES), F32),
            pltpu.VMEM((2, 8, LANES), F32),
            pltpu.VMEM((4, 8, LANES), F32),
            pltpu.SemaphoreType.DMA((rows // 8,)),
            pltpu.SemaphoreType.DMA((4,)),
            pltpu.SemaphoreType.DMA((9,)),
            pltpu.SemaphoreType.DMA((7,)),
            pltpu.SemaphoreType.DMA,
            pltpu.SemaphoreType.DMA((2,)),
        ],
        compiler_params=pltpu.CompilerParams(
            collective_id=0, has_side_effects=True, vmem_limit_bytes=32 * 1024 * 1024
        ),
        name="advance",
    )(velocity, offsets, cells, counts, moves)
    return pl.pallas_call(
        functools.partial(decode, rows, cols),
        out_shape=(
            jax.ShapeDtypeStruct((3, 1, slots), F32),
            jax.ShapeDtypeStruct((3, 1, slots), I32),
            jax.ShapeDtypeStruct((1, 1), I32),
        ),
        in_specs=[vmem],
        out_specs=(vmem, vmem, vmem),
        compiler_params=pltpu.CompilerParams(vmem_limit_bytes=1024 * 1024),
        name="decode",
    )(result)


def solution(mesh):
    placed_in = (
        P(None, None, "lat", "lon"),
        P(None, "lat", "lon"),
        P(None, "lat", "lon"),
        P("lat", "lon"),
        P("lat", "lon"),
    )
    return jax.shard_map(
        shards,
        mesh=mesh,
        in_specs=placed_in,
        out_specs=(P(None, "lat", "lon"), P(None, "lat", "lon"), P("lat", "lon")),
        check_vma=False,
    )
```

```python
import functools

import jax
import jax.numpy as jnp
from jax import lax
from jax.experimental import pallas as pl
from jax.experimental.pallas import tpu as pltpu
from jax.sharding import PartitionSpec as P

MESH = pl.DeviceIdType.MESH
CAP = 48
LANES = 128
F32, BF16, I32 = jnp.float32, jnp.bfloat16, jnp.int32
NT = (((1,), (1,)), ((), ()))
TN = (((0,), (0,)), ((), ()))


def iota(shape, dim):
    return lax.broadcasted_iota(I32, shape, dim)


def thirds(x):
    high = x.astype(BF16)
    rest = x - high.astype(F32)
    mid = rest.astype(BF16)
    low = (rest - mid.astype(F32)).astype(BF16)
    return jnp.concatenate([high.astype(F32), mid.astype(F32), low.astype(F32)], axis=0).astype(BF16)


def slots_of(target, size):
    return jnp.where(iota((size, target.shape[1]), 0) == target, 1.0, 0.0).astype(BF16)


def placed(records, onehot):
    out = lax.dot_general(thirds(records), onehot, NT, preferred_element_type=F32)
    return out[0:8] + out[8:16] + out[16:24]


def velocity_at(corners, a_row, b_row, c_row):
    sub = iota((8, a_row.shape[1]), 0)
    wb = jnp.where(sub < 4, 1.0 - b_row, b_row)
    w0 = (wb * (1.0 - c_row)).astype(BF16).astype(F32)
    w1 = (wb * c_row).astype(BF16).astype(F32)
    sums = []
    for d in range(2):
        s = w0 * corners[0][d] + w1 * corners[1][d]
        sums.append(s + pltpu.roll(s, 4, 0))
    return (1.0 - a_row) * sums[0] + a_row * sums[1]


def halo_corners(w, i_row, j_row, k_row, inside, top, sides, nrow_in, cnr_in):
    cols, rows = 2 * LANES, sides[0].shape[0]
    deep = (nrow_in.shape[0] - 16) // 2
    groups = sides[0].shape[1] // 8
    per = LANES // rows
    sub2 = iota((8, 2 * w), 0)

    def twice(x):
        return jnp.concatenate([x] * 2, axis=1)

    def hot(size, at):
        return jnp.where(iota((size, 2 * w), 0) == at, 1.0, 0.0).astype(BF16)

    k2 = jnp.concatenate([k_row, k_row + 1], axis=1)
    j2 = twice(j_row)
    outer = twice(jnp.where(i_row == cols - 1, groups, 0))
    at_side = hot(8 * groups, (k2 & (per - 1)) * (2 * groups) + outer + lax.shift_right_logical(k2, per.bit_length() - 1))
    base = twice(jnp.where(top, cols - 1 - i_row, i_row))
    second = base >= LANES
    inner = base & (LANES - 1)
    at_row = hot(2 * deep, k2 + jnp.where(second, deep, 0))
    at_level = hot(LANES, k2)

    eastern = jnp.zeros((8, 2 * w), F32)
    hits = [iota((rows, 2 * w), 0) == j2 + dj for dj in range(2)]
    for c in range(3):
        found = jnp.dot(sides[c], at_side, preferred_element_type=F32)
        for dj in range(2):
            value = jnp.sum(jnp.where(hits[dj], found, 0.0), axis=0, keepdims=True)
            eastern = jnp.where(sub2 == 4 * dj + c, value, eastern)

    few = jnp.concatenate([cnr_in[...], nrow_in[2 * deep :, 0:LANES].astype(F32)], axis=0).astype(BF16)
    ends = jnp.dot(few, at_level, preferred_element_type=F32)
    last = pltpu.roll(jnp.where(second, ends[0:8], ends[8:16]), 4, 0)

    pair = [jnp.zeros((8, 2 * w), F32), last]
    lane_id = iota((LANES, 2 * w), 0)
    hits = [lane_id == inner, lane_id == inner + 1]
    for c in range(3):
        found = lax.dot_general(
            nrow_in[0 : 2 * deep, c * LANES : (c + 1) * LANES], at_row, TN, preferred_element_type=F32
        )
        for d in range(2):
            value = jnp.sum(jnp.where(hits[d], found, 0.0), axis=0, keepdims=True)
            put = sub2 == 4 + c
            pair[d] = jnp.where(put & (inner < LANES - 1) if d else put, value, pair[d])

    sign = jnp.where(top, -1.0, 1.0)
    north = [sign * jnp.where(top, pair[1 - d], pair[d]) for d in range(2)]
    lower = iota((8, w), 0) >= 4
    corners = []
    for dk in range(2):
        part = slice(dk * w, (dk + 1) * w)
        out = []
        for d in range(2):
            here = inside[dk][d]
            if d == 1:
                here = jnp.where((i_row & (LANES - 1)) == LANES - 1, eastern[:, part], here)
            out.append(jnp.where(lower & (j_row == rows - 1), north[d][:, part], here))
        corners.append(out)
    return corners


def advanced(corners, position):
    first = velocity_at(corners, position[0:1], position[1:2], position[2:3])
    middle = position + 0.5 * first
    return position + velocity_at(corners, middle[0:1], middle[1:2], middle[2:3])


def kernel(
    dims, vel_hbm, off_hbm, cell_hbm, count_hbm, move_hbm,
    out_ref,
    vel, off_ref, cell_ref, move_ref, count_ref, table, where_ref, where_smem, first_ref, first_smem,
    gathered, first_gathered, stay_ref,
    side, column, nrow, nfold, cnr, cfold, col_in, nrow_in, cnr_in,
    pack, pack_in, vsem, isem, send, recv, lsem, asem,
):
    depth, rows, cols, slots, live, n_lat, n_lon = dims
    wide = pl.cdiv(live, LANES) * LANES
    tiles = wide // LANES
    half = LANES // 2
    few = 4 * half
    level = rows * 4
    span = table.shape[0] // 2
    deep = span // level
    per = LANES // rows
    groups = side.shape[1]
    r, p = lax.axis_index("lat"), lax.axis_index("lon")
    east, west = lax.rem(p + 1, n_lon), lax.rem(p + n_lon - 1, n_lon)
    across, corner = n_lon - 1 - p, lax.rem(n_lon - p, n_lon)
    top = r == n_lat - 1
    away = jnp.logical_and(top, corner != p)

    smalls = [(cell_hbm, cell_ref), (move_hbm, move_ref), (count_hbm, count_ref), (off_hbm, off_ref)]
    smalls = [pltpu.make_async_copy(src, dst, isem.at[n]) for n, (src, dst) in enumerate(smalls)]
    bands = [slice(8 * n, 8 * n + 8) for n in range(rows // 8)]
    bands = [bands[0], bands[-1]] + bands[1:-1]
    loads = [
        pltpu.make_async_copy(vel_hbm.at[:, :, band, :], vel.at[:, :, band, :], vsem.at[n])
        for n, band in enumerate(bands)
    ]
    loads[0].start()
    for copy in smalls + loads[1:]:
        copy.start()

    barrier = pltpu.get_barrier_semaphore()

    def greet(lat, lon):
        pl.semaphore_signal(barrier, inc=1, device_id=(lon, lat), device_id_type=MESH)

    greet(r, east)
    greet(r, west)

    @pl.when(r < n_lat - 1)
    def _():
        greet(r + 1, p)
        greet(r + 1, east)

    @pl.when(r > 0)
    def _():
        greet(r - 1, p)

    @pl.when(top)
    def _():
        greet(r, across)

    @pl.when(away)
    def _():
        greet(r, corner)

    lane = iota((8, LANES), 1)
    sub = iota((8, wide), 0)
    for part in range(2):
        table[pl.ds(part * span + depth * level, span - depth * level), :] = jnp.zeros(
            (span - depth * level, LANES), F32
        )
    side[...] = jnp.zeros_like(side)
    gathered[...] = jnp.zeros_like(gathered)
    first_gathered[...] = jnp.zeros_like(first_gathered)
    first_lane = jnp.where(lane == 0, 1.0, 0.0).astype(BF16)

    def build(n):
        band = bands[n]
        loads[n].wait()

        def body(step, carry):
            for u in range(5):
                k = step * 5 + u
                for c in range(3):
                    for h in range(2):
                        at = h * span + k * level + 4 * band.start + c
                        table[pl.ds(at, 8, stride=4), :] = vel[c, k, band, h * LANES : (h + 1) * LANES].astype(F32)
            return carry

        lax.fori_loop(0, depth // 5, body, 0)

    def edge(target, ends, row):
        firsts = [jnp.zeros((8, deep), F32)] * 2
        for h in range(2):
            for c in range(3):
                blocks = []
                for block in range(deep // 8):
                    at = h * span + block * 8 * level + 4 * row + c
                    blocks.append(table[pl.ds(at, 8, stride=level), :])
                plane = jnp.concatenate(blocks, axis=0).astype(BF16)
                target[pl.ds(h * deep, deep), pl.ds(c * LANES, LANES)] = plane
                pick = jnp.where((lane == 0) & (iota((8, LANES), 0) == c), 1.0, 0.0).astype(BF16)
                firsts[h] = firsts[h] + lax.dot_general(pick, plane, NT, preferred_element_type=F32)
        pad = jnp.zeros((8, LANES - deep), F32)
        tail = jnp.concatenate([jnp.concatenate([firsts[1], pad], axis=1), jnp.zeros((8, LANES), F32)], axis=0)
        target[2 * deep : 2 * deep + 16, :] = jnp.concatenate([tail, jnp.zeros((16, 2 * LANES), F32)], axis=1).astype(BF16)
        ends[...] = jnp.concatenate([firsts[0], pad], axis=1)

    def remote(src, dst, s, t, lat, lon):
        return pltpu.make_async_remote_copy(
            src, dst, send.at[s], recv.at[t], device_id=(lon, lat), device_id_type=MESH
        )

    col_out = remote(column, col_in, 0, 0, r, west)
    row_out = remote(nrow, nrow_in, 1, 1, r - 1, p)
    cnr_out = remote(cnr, cnr_in, 2, 2, r - 1, west)
    fold_out = remote(nfold, nrow_in, 3, 1, r, across)
    cfold_out = remote(cfold, cnr_in, 4, 2, r, corner)
    cfold_here = pltpu.make_async_copy(cfold, cnr_in, lsem)

    build(0)
    edge(nrow, cnr, 0)
    peers = 2 + 2 * (r > 0).astype(I32) + (r < n_lat - 1).astype(I32) + top.astype(I32) + away.astype(I32)

    def send_rows():
        pl.semaphore_wait(barrier, peers)

        @pl.when(r > 0)
        def _():
            cnr_out.start()
            row_out.start()

    def send_fold():
        @pl.when(top)
        def _():
            fold_out.start()

        @pl.when(away)
        def _():
            cfold_out.start()

    patient = p == 0
    eager = jnp.logical_not(patient)

    @pl.when(eager)
    def _():
        send_rows()

    for small in smalls:
        small.wait()

    i_row, j_row, k_row = (cell_ref[n, :, 0:wide] for n in range(3))
    motion = move_ref[:, 0:wide]
    valid = iota((1, wide), 1) < count_ref[...]
    chosen = jnp.where((sub == motion) & valid, 1.0, 0.0)
    before = jnp.where(iota((LANES, LANES), 0) < iota((LANES, LANES), 1), 1.0, 0.0).astype(BF16)
    upto = jnp.concatenate([before, jnp.ones((LANES, LANES), BF16)], axis=1)

    def ranked(flags, total):
        out = []
        for t in range(flags.shape[1] // LANES):
            sums = jnp.dot(
                flags[:, t * LANES : (t + 1) * LANES].astype(BF16), upto, preferred_element_type=F32
            )
            out.append(sums[:, :LANES] + total)
            total = total + sums[:, LANES:]
        return jnp.concatenate(out, axis=1), total

    rank, total = ranked(chosen, jnp.zeros((8, LANES), F32))
    stay_to = jnp.where(chosen[0:1] > 0.5, rank[0:1], -1.0).astype(I32)
    slot_to = rank + (half * (sub - 1)).astype(F32)
    leaving = (sub >= 1) & (chosen > 0.5)
    leave_to = (jnp.sum(jnp.where(leaving, slot_to + 1.0, 0.0), axis=0, keepdims=True) - 1.0).astype(I32)
    position = jnp.zeros((8, wide), F32)
    for n in range(3):
        position = jnp.where(sub == n, off_ref[n, :, 0:wide], position)
    marks = jnp.where(sub == 0, i_row, jnp.where(sub == 1, j_row, jnp.where(sub == 2, k_row, 1)))
    raw = lax.dot_general(
        jnp.concatenate([thirds(position).astype(F32), marks.astype(F32)], axis=0).astype(BF16),
        slots_of(leave_to, few), NT, preferred_element_type=F32,
    )
    first_position = raw[0:8] + raw[8:16] + raw[16:24]
    first_i, first_j, first_k = (
        jnp.clip(raw[24 + n : 25 + n].astype(I32), 0, top_value)
        for n, top_value in enumerate((cols - 1, rows - 1, depth - 2))
    )
    first_real = raw[27:28] > 0.5

    def words(i, j, k, target):
        start = jnp.where(i >= LANES, span, 0) + k * level + 4 * j
        start = start * LANES + ((iota(i.shape, 1) - i) & (LANES - 1))
        for t in range(i.shape[1] // LANES):
            part = start[:, t * LANES : (t + 1) * LANES]
            target[2 * t : 2 * t + 1, :] = part
            target[2 * t + 1 : 2 * t + 2, :] = pltpu.roll(part, half, 1)

    words(first_i, first_j, first_k, first_ref)
    words(i_row, j_row, k_row, where_ref)
    addresses = [
        pltpu.make_async_copy(first_ref, first_smem, asem.at[0]),
        pltpu.make_async_copy(where_ref, where_smem, asem.at[1]),
    ]
    for copy in addresses:
        copy.start()
    stay_ref[...] = slots_of(stay_to, wide)

    build(1)

    @pl.when(top)
    def _():
        edge(nfold, cfold, rows - 1)

    @pl.when(eager)
    def _():
        send_fold()

    @pl.when(jnp.logical_and(top, corner == p))
    def _():
        cfold_here.start()

    for n in range(2, len(bands)):
        build(n)

    for c in range(3):
        for h in range(2):
            plane = vel[c, :, :, h * LANES : (h + 1) * LANES].reshape(depth * rows, LANES)
            line = lax.dot_general(first_lane, plane, NT, preferred_element_type=F32)[0:1]
            for g in range(pl.cdiv(depth, per)):
                n = min(LANES, depth * rows - g * LANES)
                side[h * 3 + c, g : g + 1, 0:n] = line[:, g * LANES : g * LANES + n]
    column[...] = side[0:3].astype(BF16)
    @pl.when(eager)
    def _():
        col_out.start()

    def gather(source, target, count):
        def body(step, carry):
            base = (step & 1) * half
            group = step >> 1
            ahead = lane - base
            accs = [target[n, group] for n in range(4)]
            for u in range(count):
                word = source[step, u]
                at, shift = word >> 7, word & (LANES - 1)
                here = ahead == u
                there = ahead == u + 1 if u < half - 1 else lane == ((base + half) & (LANES - 1))
                for dk in range(2):
                    turned = pltpu.roll(table[pl.ds(at + dk * level, 8), :], shift, 1)
                    accs[2 * dk] = jnp.where(here, turned, accs[2 * dk])
                    accs[2 * dk + 1] = jnp.where(there, turned, accs[2 * dk + 1])
            for n in range(4):
                target[n, group] = accs[n]
            return carry

        return body

    def together(source, w):
        out = []
        for dk in range(2):
            low = [source[2 * dk, t] for t in range(w // LANES)]
            high = [pltpu.roll(source[2 * dk + 1, t], LANES - 1, 1) for t in range(w // LANES)]
            out.append([jnp.concatenate(low, axis=1), jnp.concatenate(high, axis=1)])
        return out

    for copy in addresses:
        copy.wait()
    lax.fori_loop(0, 4, gather(first_smem, first_gathered, CAP), 0)
    lax.fori_loop(0, live // half, gather(where_smem, gathered, half), 0)

    @pl.when(patient)
    def _():
        send_rows()
        send_fold()
        col_out.start()


    go = iota((1, few), 1) // half + 1
    folding = (go == 3) & top
    last_i, last_j = cols - 1, rows - 1
    new_i = jnp.where(
        go == 1, 0, jnp.where(go == 2, last_i, jnp.where(folding, last_i - first_i, first_i))
    )
    new_j = jnp.where(
        go == 3, jnp.where(top, last_j, 0), jnp.where(go == 4, last_j, first_j)
    )
    code = jnp.where(first_real, 1 + new_i + cols * (new_j + rows * first_k), 0).astype(F32)

    cnr_wait = remote(cnr, cnr_in, 2, 2, r, west)
    col_out.wait_recv()
    row_out.wait_recv()

    @pl.when(jnp.logical_or(jnp.logical_not(top), corner != p))
    def _():
        cnr_wait.wait_recv()

    @pl.when(jnp.logical_and(top, corner == p))
    def _():
        cfold_here.wait()

    sides = []
    for c in range(3):
        lines = jnp.concatenate([side[3 + c], col_in[c].astype(F32)], axis=0)
        lines = [lines if m == 0 else pltpu.roll(lines, LANES - m * rows, 1) for m in range(per)]
        sides.append(jnp.concatenate(lines, axis=0).T[0:rows].astype(BF16))

    corners = halo_corners(
        few, first_i, first_j, first_k, together(first_gathered, few), top, sides, nrow_in, cnr_in
    )
    moved = advanced(corners, first_position)
    na, nb, nc = moved[0:1], moved[1:2], moved[2:3]
    new_a = jnp.where(go == 1, na - 1.0, jnp.where(go == 2, na + 1.0, jnp.where(folding, 1.0 - na, na)))
    new_b = jnp.where(go == 3, jnp.where(top, 2.0 - nb, nb - 1.0), jnp.where(go == 4, nb + 1.0, nb))
    sub_few = iota((8, few), 0)
    records = jnp.where(
        sub_few == 0, new_a,
        jnp.where(sub_few == 1, new_b, jnp.where(sub_few == 2, nc, jnp.where(sub_few == 3, code, 0.0))),
    )
    records = jnp.where(first_real, records, 0.0)

    for m in range(2):
        pack[m] = records[:, m * LANES : (m + 1) * LANES]

    @pl.when(r == 0)
    def _():
        pack_in[2] = jnp.zeros((8, LANES), F32)

    east_out = remote(pack.at[0], pack_in.at[0], 5, 3, r, east)
    west_out = remote(pack.at[0], pack_in.at[1], 6, 4, r, west)
    north_out = remote(pack.at[1], pack_in.at[2], 7, 5, r + 1, p)
    over_out = remote(pack.at[1], pack_in.at[3], 7, 6, r, across)
    south_out = remote(pack.at[1], pack_in.at[3], 8, 6, r - 1, p)

    @pl.when(top)
    def _():
        over_out.start()

    @pl.when(r < n_lat - 1)
    def _():
        north_out.start()

    @pl.when(r > 0)
    def _():
        south_out.start()

    east_out.start()
    west_out.start()

    corners = halo_corners(
        wide, i_row, j_row, k_row, together(gathered, wide), top, sides, nrow_in, cnr_in
    )
    moved = advanced(corners, position)
    code = (1 + i_row + cols * (j_row + rows * k_row)).astype(F32)
    kept = placed(jnp.where(sub < 3, moved, jnp.where(sub == 3, code, 0.0)), stay_ref[...])

    east_out.wait_recv()
    west_out.wait_recv()

    @pl.when(r > 0)
    def _():
        north_out.wait_recv()

    over_out.wait_recv()

    from_north = jnp.where(top, pltpu.roll(pack_in[3], half, 1), pack_in[3])
    arrivals = jnp.concatenate(
        [
            jnp.where(lane < half, pack_in[0], pack_in[1]),
            jnp.where(lane < half, pack_in[2], from_north),
        ],
        axis=1,
    )
    present = jnp.where(arrivals > 0.5, 1.0, 0.0)
    order, filled = ranked(present, jnp.broadcast_to(total[0:1], (8, LANES)))
    arrive_to = jnp.where(present[3:4] > 0.5, order[3:4], -1.0).astype(I32)
    joined = placed(arrivals, slots_of(arrive_to, slots))
    result = joined + jnp.concatenate([kept, jnp.zeros((8, slots - wide), F32)], axis=1)
    out_ref[...] = jnp.where(iota((8, slots), 0) == 4, filled[3:4, 0:1], result)

    col_out.wait_send()
    east_out.wait_send()
    west_out.wait_send()
    north_out.wait_send()

    @pl.when(r > 0)
    def _():
        row_out.wait_send()
        cnr_out.wait_send()
        south_out.wait_send()

    @pl.when(top)
    def _():
        fold_out.wait_send()

    @pl.when(away)
    def _():
        cfold_out.wait_send()


def decode(rows, cols, result_ref, new_off, new_cell, new_count):
    for n in range(3):
        new_off[n] = result_ref[n : n + 1, :]
    code = jnp.maximum(result_ref[3:4, :].astype(I32) - 1, 0)
    new_cell[0] = code & (cols - 1)
    new_cell[1] = (code // cols) & (rows - 1)
    new_cell[2] = code // (cols * rows)
    new_count[...] = result_ref[4:5, 0:1].astype(I32)


def shards(velocity, offsets, cells, counts, moves):
    _, depth, rows, cols = velocity.shape
    slots = offsets.shape[2]
    live = slots * 3 // 4
    wide = pl.cdiv(live, LANES) * LANES
    deep = pl.cdiv(depth, 16) * 16
    dims = (depth, rows, cols, slots, live, lax.axis_size("lat"), lax.axis_size("lon"))
    groups = pl.cdiv(depth * rows, 8 * LANES) * 8
    vmem = pl.BlockSpec(memory_space=pltpu.VMEM)
    hbm = pl.BlockSpec(memory_space=pltpu.HBM)
    velocity, offsets, cells, moves = (
        pltpu.with_memory_space_constraint(x, pltpu.HBM) for x in (velocity, offsets, cells, moves)
    )
    result = pl.pallas_call(
        functools.partial(kernel, dims),
        out_shape=jax.ShapeDtypeStruct((8, slots), F32),
        in_specs=[hbm] * 5,
        out_specs=vmem,
        scratch_shapes=[
            pltpu.VMEM((3, depth, rows, cols), BF16),
            pltpu.VMEM((3, 1, slots), F32),
            pltpu.VMEM((3, 1, slots), I32),
            pltpu.VMEM((1, slots), I32),
            pltpu.VMEM((1, 1), I32),
            pltpu.VMEM((2 * deep * rows * 4, LANES), F32),
            pltpu.VMEM((2 * wide // LANES, LANES), I32),
            pltpu.SMEM((2 * wide // LANES, LANES), I32),
            pltpu.VMEM((4, LANES), I32),
            pltpu.SMEM((4, LANES), I32),
            pltpu.VMEM((4, wide // LANES, 8, LANES), F32),
            pltpu.VMEM((4, 2, 8, LANES), F32),
            pltpu.VMEM((wide, wide), BF16),
            pltpu.VMEM((6, groups, LANES), F32),
            pltpu.VMEM((3, groups, LANES), BF16),
            pltpu.VMEM((2 * deep + 16, 3 * LANES), BF16),
            pltpu.VMEM((2 * deep + 16, 3 * LANES), BF16),
            pltpu.VMEM((8, LANES), F32),
            pltpu.VMEM((8, LANES), F32),
            pltpu.VMEM((3, groups, LANES), BF16),
            pltpu.VMEM((2 * deep + 16, 3 * LANES), BF16),
            pltpu.VMEM((8, LANES), F32),
            pltpu.VMEM((2, 8, LANES), F32),
            pltpu.VMEM((4, 8, LANES), F32),
            pltpu.SemaphoreType.DMA((rows // 8,)),
            pltpu.SemaphoreType.DMA((4,)),
            pltpu.SemaphoreType.DMA((9,)),
            pltpu.SemaphoreType.DMA((7,)),
            pltpu.SemaphoreType.DMA,
            pltpu.SemaphoreType.DMA((2,)),
        ],
        compiler_params=pltpu.CompilerParams(
            collective_id=0, has_side_effects=True, vmem_limit_bytes=32 * 1024 * 1024
        ),
        name="advance",
    )(velocity, offsets, cells, counts, moves)
    return pl.pallas_call(
        functools.partial(decode, rows, cols),
        out_shape=(
            jax.ShapeDtypeStruct((3, 1, slots), F32),
            jax.ShapeDtypeStruct((3, 1, slots), I32),
            jax.ShapeDtypeStruct((1, 1), I32),
        ),
        in_specs=[vmem],
        out_specs=(vmem, vmem, vmem),
        compiler_params=pltpu.CompilerParams(vmem_limit_bytes=1024 * 1024),
        name="decode",
    )(result)


def solution(mesh):
    placed_in = (
        P(None, None, "lat", "lon"),
        P(None, "lat", "lon"),
        P(None, "lat", "lon"),
        P("lat", "lon"),
        P("lat", "lon"),
    )
    return jax.shard_map(
        shards,
        mesh=mesh,
        in_specs=placed_in,
        out_specs=(P(None, "lat", "lon"), P(None, "lat", "lon"), P("lat", "lon")),
        check_vma=False,
    )
```

```python
import functools

import jax
import jax.numpy as jnp
from jax import lax
from jax.experimental import pallas as pl
from jax.experimental.pallas import tpu as pltpu
from jax.sharding import PartitionSpec as P

MESH = pl.DeviceIdType.MESH
CAP = 48
LANES = 128
F32, BF16, I32 = jnp.float32, jnp.bfloat16, jnp.int32
NT = (((1,), (1,)), ((), ()))
TN = (((0,), (0,)), ((), ()))


def iota(shape, dim):
    return lax.broadcasted_iota(I32, shape, dim)


def thirds(x):
    high = x.astype(BF16)
    rest = x - high.astype(F32)
    mid = rest.astype(BF16)
    low = (rest - mid.astype(F32)).astype(BF16)
    return jnp.concatenate([high.astype(F32), mid.astype(F32), low.astype(F32)], axis=0).astype(BF16)


def slots_of(target, size):
    return jnp.where(iota((size, target.shape[1]), 0) == target, 1.0, 0.0).astype(BF16)


def placed(records, onehot):
    out = lax.dot_general(thirds(records), onehot, NT, preferred_element_type=F32)
    return out[0:8] + out[8:16] + out[16:24]


def velocity_at(corners, a_row, b_row, c_row):
    sub = iota((8, a_row.shape[1]), 0)
    wb = jnp.where(sub < 4, 1.0 - b_row, b_row)
    w0 = (wb * (1.0 - c_row)).astype(BF16).astype(F32)
    w1 = (wb * c_row).astype(BF16).astype(F32)
    sums = []
    for d in range(2):
        s = w0 * corners[0][d] + w1 * corners[1][d]
        sums.append(s + pltpu.roll(s, 4, 0))
    return (1.0 - a_row) * sums[0] + a_row * sums[1]


def halo_corners(w, i_row, j_row, k_row, inside, top, sides, nrow_in, cnr_in):
    cols, rows = 2 * LANES, sides[0].shape[0]
    deep = (nrow_in.shape[0] - 16) // 2
    groups = sides[0].shape[1] // 8
    per = LANES // rows
    sub2 = iota((8, 2 * w), 0)

    def twice(x):
        return jnp.concatenate([x] * 2, axis=1)

    def hot(size, at):
        return jnp.where(iota((size, 2 * w), 0) == at, 1.0, 0.0).astype(BF16)

    k2 = jnp.concatenate([k_row, k_row + 1], axis=1)
    j2 = twice(j_row)
    outer = twice(jnp.where(i_row == cols - 1, groups, 0))
    at_side = hot(8 * groups, (k2 & (per - 1)) * (2 * groups) + outer + lax.shift_right_logical(k2, per.bit_length() - 1))
    base = twice(jnp.where(top, cols - 1 - i_row, i_row))
    second = base >= LANES
    inner = base & (LANES - 1)
    at_row = hot(2 * deep, k2 + jnp.where(second, deep, 0))
    at_level = hot(LANES, k2)

    eastern = jnp.zeros((8, 2 * w), F32)
    hits = [iota((rows, 2 * w), 0) == j2 + dj for dj in range(2)]
    for c in range(3):
        found = jnp.dot(sides[c], at_side, preferred_element_type=F32)
        for dj in range(2):
            value = jnp.sum(jnp.where(hits[dj], found, 0.0), axis=0, keepdims=True)
            eastern = jnp.where(sub2 == 4 * dj + c, value, eastern)

    few = jnp.concatenate([cnr_in[...], nrow_in[2 * deep :, 0:LANES].astype(F32)], axis=0).astype(BF16)
    ends = jnp.dot(few, at_level, preferred_element_type=F32)
    last = pltpu.roll(jnp.where(second, ends[0:8], ends[8:16]), 4, 0)

    pair = [jnp.zeros((8, 2 * w), F32), last]
    lane_id = iota((LANES, 2 * w), 0)
    hits = [lane_id == inner, lane_id == inner + 1]
    for c in range(3):
        found = lax.dot_general(
            nrow_in[0 : 2 * deep, c * LANES : (c + 1) * LANES], at_row, TN, preferred_element_type=F32
        )
        for d in range(2):
            value = jnp.sum(jnp.where(hits[d], found, 0.0), axis=0, keepdims=True)
            put = sub2 == 4 + c
            pair[d] = jnp.where(put & (inner < LANES - 1) if d else put, value, pair[d])

    sign = jnp.where(top, -1.0, 1.0)
    north = [sign * jnp.where(top, pair[1 - d], pair[d]) for d in range(2)]
    lower = iota((8, w), 0) >= 4
    corners = []
    for dk in range(2):
        part = slice(dk * w, (dk + 1) * w)
        out = []
        for d in range(2):
            here = inside[dk][d]
            if d == 1:
                here = jnp.where((i_row & (LANES - 1)) == LANES - 1, eastern[:, part], here)
            out.append(jnp.where(lower & (j_row == rows - 1), north[d][:, part], here))
        corners.append(out)
    return corners


def advanced(corners, position):
    first = velocity_at(corners, position[0:1], position[1:2], position[2:3])
    middle = position + 0.5 * first
    return position + velocity_at(corners, middle[0:1], middle[1:2], middle[2:3])


def kernel(
    dims, vel_hbm, off_hbm, cell_hbm, count_hbm, move_hbm,
    out_ref,
    vel, off_ref, cell_ref, move_ref, count_ref, table, where_ref, where_smem, first_ref, first_smem,
    gathered, first_gathered, stay_ref,
    side, column, nrow, nfold, cnr, cfold, col_in, nrow_in, cnr_in,
    pack, pack_in, vsem, isem, send, recv, lsem, asem,
):
    depth, rows, cols, slots, live, n_lat, n_lon = dims
    wide = pl.cdiv(live, LANES) * LANES
    tiles = wide // LANES
    half = LANES // 2
    few = 4 * half
    level = rows * 4
    deep = pl.cdiv(depth, 16) * 16
    span = deep * level
    per = LANES // rows
    groups = side.shape[1]
    r, p = lax.axis_index("lat"), lax.axis_index("lon")
    east, west = lax.rem(p + 1, n_lon), lax.rem(p + n_lon - 1, n_lon)
    across, corner = n_lon - 1 - p, lax.rem(n_lon - p, n_lon)
    top = r == n_lat - 1
    away = jnp.logical_and(top, corner != p)

    smalls = [(cell_hbm, cell_ref), (move_hbm, move_ref), (count_hbm, count_ref), (off_hbm, off_ref)]
    smalls = [pltpu.make_async_copy(src, dst, isem.at[n]) for n, (src, dst) in enumerate(smalls)]
    bands = [slice(8 * n, 8 * n + 8) for n in range(rows // 8)]
    bands = [bands[0], bands[-1]] + bands[1:-1]
    loads = [
        pltpu.make_async_copy(vel_hbm.at[:, :, band, :], vel.at[:, :, band, :], vsem.at[n])
        for n, band in enumerate(bands)
    ]
    loads[0].start()
    for copy in smalls + loads[1:]:
        copy.start()

    barrier = pltpu.get_barrier_semaphore()

    def greet(lat, lon):
        pl.semaphore_signal(barrier, inc=1, device_id=(lon, lat), device_id_type=MESH)

    greet(r, east)
    greet(r, west)

    @pl.when(r < n_lat - 1)
    def _():
        greet(r + 1, p)
        greet(r + 1, east)

    @pl.when(r > 0)
    def _():
        greet(r - 1, p)

    @pl.when(top)
    def _():
        greet(r, across)

    @pl.when(away)
    def _():
        greet(r, corner)

    lane = iota((8, LANES), 1)
    sub = iota((8, wide), 0)
    for part in range(2):
        table[pl.ds(part * span + depth * level, span - depth * level), :] = jnp.zeros(
            (span - depth * level, LANES), F32
        )
    side[...] = jnp.zeros_like(side)
    gathered[...] = jnp.zeros_like(gathered)
    first_gathered[...] = jnp.zeros_like(first_gathered)
    first_lane = jnp.where(lane == 0, 1.0, 0.0).astype(BF16)

    def build(n):
        band = bands[n]
        loads[n].wait()

        def body(step, carry):
            for u in range(5):
                k = step * 5 + u
                for c in range(3):
                    for h in range(2):
                        at = h * span + k * level + 4 * band.start + c
                        table[pl.ds(at, 8, stride=4), :] = vel[c, k, band, h * LANES : (h + 1) * LANES].astype(F32)
            return carry

        lax.fori_loop(0, depth // 5, body, 0)

    def edge(target, ends, row):
        firsts = [jnp.zeros((8, deep), F32)] * 2
        for h in range(2):
            for c in range(3):
                blocks = []
                for block in range(deep // 8):
                    at = h * span + block * 8 * level + 4 * row + c
                    blocks.append(table[pl.ds(at, 8, stride=level), :])
                plane = jnp.concatenate(blocks, axis=0).astype(BF16)
                target[pl.ds(h * deep, deep), pl.ds(c * LANES, LANES)] = plane
                pick = jnp.where((lane == 0) & (iota((8, LANES), 0) == c), 1.0, 0.0).astype(BF16)
                firsts[h] = firsts[h] + lax.dot_general(pick, plane, NT, preferred_element_type=F32)
        pad = jnp.zeros((8, LANES - deep), F32)
        tail = jnp.concatenate([jnp.concatenate([firsts[1], pad], axis=1), jnp.zeros((8, LANES), F32)], axis=0)
        target[2 * deep : 2 * deep + 16, :] = jnp.concatenate([tail, jnp.zeros((16, 2 * LANES), F32)], axis=1).astype(BF16)
        ends[...] = jnp.concatenate([firsts[0], pad], axis=1)

    def remote(src, dst, s, t, lat, lon):
        return pltpu.make_async_remote_copy(
            src, dst, send.at[s], recv.at[t], device_id=(lon, lat), device_id_type=MESH
        )

    col_out = remote(column, col_in, 0, 0, r, west)
    row_out = remote(nrow, nrow_in, 1, 1, r - 1, p)
    cnr_out = remote(cnr, cnr_in, 2, 2, r - 1, west)
    fold_out = remote(nfold, nrow_in, 3, 1, r, across)
    cfold_out = remote(cfold, cnr_in, 4, 2, r, corner)
    cfold_here = pltpu.make_async_copy(cfold, cnr_in, lsem)

    build(0)
    edge(nrow, cnr, 0)
    peers = 2 + 2 * (r > 0).astype(I32) + (r < n_lat - 1).astype(I32) + top.astype(I32) + away.astype(I32)

    def send_rows(*first):
        pl.semaphore_wait(barrier, peers)
        for copy in first:
            copy.start()

        @pl.when(r > 0)
        def _():
            cnr_out.start()
            row_out.start()

    def send_fold():
        @pl.when(top)
        def _():
            fold_out.start()

        @pl.when(away)
        def _():
            cfold_out.start()

    patient = p == 0
    eager = jnp.logical_not(patient)

    @pl.when(eager)
    def _():
        send_rows()

    for small in smalls:
        small.wait()

    i_row, j_row, k_row = (cell_ref[n, :, 0:wide] for n in range(3))
    motion = move_ref[:, 0:wide]
    valid = iota((1, wide), 1) < count_ref[...]
    chosen = jnp.where((sub == motion) & valid, 1.0, 0.0)
    before = jnp.where(iota((LANES, LANES), 0) < iota((LANES, LANES), 1), 1.0, 0.0).astype(BF16)
    upto = jnp.concatenate([before, jnp.ones((LANES, LANES), BF16)], axis=1)

    def ranked(flags, total):
        out = []
        for t in range(flags.shape[1] // LANES):
            sums = jnp.dot(
                flags[:, t * LANES : (t + 1) * LANES].astype(BF16), upto, preferred_element_type=F32
            )
            out.append(sums[:, :LANES] + total)
            total = total + sums[:, LANES:]
        return jnp.concatenate(out, axis=1), total

    rank, total = ranked(chosen, jnp.zeros((8, LANES), F32))
    stay_to = jnp.where(chosen[0:1] > 0.5, rank[0:1], -1.0).astype(I32)
    slot_to = rank + (half * (sub - 1)).astype(F32)
    leaving = (sub >= 1) & (chosen > 0.5)
    leave_to = (jnp.sum(jnp.where(leaving, slot_to + 1.0, 0.0), axis=0, keepdims=True) - 1.0).astype(I32)
    position = jnp.zeros((8, wide), F32)
    for n in range(3):
        position = jnp.where(sub == n, off_ref[n, :, 0:wide], position)
    marks = jnp.where(sub == 0, i_row, jnp.where(sub == 1, j_row, jnp.where(sub == 2, k_row, 1)))
    raw = lax.dot_general(
        jnp.concatenate([thirds(position).astype(F32), marks.astype(F32)], axis=0).astype(BF16),
        slots_of(leave_to, few), NT, preferred_element_type=F32,
    )
    first_position = raw[0:8] + raw[8:16] + raw[16:24]
    first_i, first_j, first_k = (
        jnp.clip(raw[24 + n : 25 + n].astype(I32), 0, top_value)
        for n, top_value in enumerate((cols - 1, rows - 1, depth - 2))
    )
    first_real = raw[27:28] > 0.5

    def words(i, j, k, target):
        start = jnp.clip(jnp.where(i >= LANES, span, 0) + k * level + 4 * j, 0, 2 * span - level - 8)
        start = start * LANES + ((iota(i.shape, 1) - i) & (LANES - 1))
        for t in range(i.shape[1] // LANES):
            part = start[:, t * LANES : (t + 1) * LANES]
            target[2 * t : 2 * t + 1, :] = part
            target[2 * t + 1 : 2 * t + 2, :] = pltpu.roll(part, half, 1)

    first_ref[...] = jnp.zeros_like(first_ref)
    where_ref[...] = jnp.zeros_like(where_ref)
    words(first_i, first_j, first_k, first_ref)
    words(i_row, j_row, k_row, where_ref)
    addresses = [
        pltpu.make_async_copy(first_ref, first_smem, asem.at[0]),
        pltpu.make_async_copy(where_ref, where_smem, asem.at[1]),
    ]
    for copy in addresses:
        copy.start()
    stay_ref[...] = slots_of(stay_to, wide)

    build(1)

    @pl.when(top)
    def _():
        edge(nfold, cfold, rows - 1)

    @pl.when(eager)
    def _():
        send_fold()

    @pl.when(jnp.logical_and(top, corner == p))
    def _():
        cfold_here.start()

    for n in range(2, len(bands)):
        build(n)

    for c in range(3):
        for h in range(2):
            plane = vel[c, :, :, h * LANES : (h + 1) * LANES].reshape(depth * rows, LANES)
            line = lax.dot_general(first_lane, plane, NT, preferred_element_type=F32)[0:1]
            for g in range(pl.cdiv(depth, per)):
                n = min(LANES, depth * rows - g * LANES)
                side[h * 3 + c, g : g + 1, 0:n] = line[:, g * LANES : g * LANES + n]
    column[...] = side[0:3].astype(BF16)
    @pl.when(eager)
    def _():
        col_out.start()

    def gather(source, target, count):
        def body(step, carry):
            base = (step & 1) * half
            group = step >> 1
            ahead = lane - base
            accs = [target[n, group] for n in range(4)]
            for u in range(count):
                word = source[step, u]
                at, shift = word >> 7, word & (LANES - 1)
                here = ahead == u
                there = ahead == u + 1 if u < half - 1 else lane == ((base + half) & (LANES - 1))
                for dk in range(2):
                    turned = pltpu.roll(table[pl.ds(at + dk * level, 8), :], shift, 1)
                    accs[2 * dk] = jnp.where(here, turned, accs[2 * dk])
                    accs[2 * dk + 1] = jnp.where(there, turned, accs[2 * dk + 1])
            for n in range(4):
                target[n, group] = accs[n]
            return carry

        return body

    def together(source, w):
        out = []
        for dk in range(2):
            low = [source[2 * dk, t] for t in range(w // LANES)]
            high = [pltpu.roll(source[2 * dk + 1, t], LANES - 1, 1) for t in range(w // LANES)]
            out.append([jnp.concatenate(low, axis=1), jnp.concatenate(high, axis=1)])
        return out

    for copy in addresses:
        copy.wait()
    lax.fori_loop(0, 4, gather(first_smem, first_gathered, CAP), 0)

    later = (r % 2 == 0) & (p > 0)

    def gather_rest():
        lax.fori_loop(0, live // half, gather(where_smem, gathered, half), 0)

    @pl.when(jnp.logical_not(later))
    def _():
        gather_rest()

    @pl.when(patient)
    def _():
        send_rows(col_out)
        send_fold()


    go = iota((1, few), 1) // half + 1
    folding = (go == 3) & top
    last_i, last_j = cols - 1, rows - 1
    new_i = jnp.where(
        go == 1, 0, jnp.where(go == 2, last_i, jnp.where(folding, last_i - first_i, first_i))
    )
    new_j = jnp.where(
        go == 3, jnp.where(top, last_j, 0), jnp.where(go == 4, last_j, first_j)
    )
    code = jnp.where(first_real, 1 + new_i + cols * (new_j + rows * first_k), 0).astype(F32)

    cnr_wait = remote(cnr, cnr_in, 2, 2, r, west)
    col_out.wait_recv()
    row_out.wait_recv()

    @pl.when(jnp.logical_or(jnp.logical_not(top), corner != p))
    def _():
        cnr_wait.wait_recv()

    @pl.when(jnp.logical_and(top, corner == p))
    def _():
        cfold_here.wait()

    sides = []
    for c in range(3):
        lines = jnp.concatenate([side[3 + c], col_in[c].astype(F32)], axis=0)
        lines = [lines if m == 0 else pltpu.roll(lines, LANES - m * rows, 1) for m in range(per)]
        sides.append(jnp.concatenate(lines, axis=0).T[0:rows].astype(BF16))

    corners = halo_corners(
        few, first_i, first_j, first_k, together(first_gathered, few), top, sides, nrow_in, cnr_in
    )
    moved = advanced(corners, first_position)
    na, nb, nc = moved[0:1], moved[1:2], moved[2:3]
    new_a = jnp.where(go == 1, na - 1.0, jnp.where(go == 2, na + 1.0, jnp.where(folding, 1.0 - na, na)))
    new_b = jnp.where(go == 3, jnp.where(top, 2.0 - nb, nb - 1.0), jnp.where(go == 4, nb + 1.0, nb))
    sub_few = iota((8, few), 0)
    records = jnp.where(
        sub_few == 0, new_a,
        jnp.where(sub_few == 1, new_b, jnp.where(sub_few == 2, nc, jnp.where(sub_few == 3, code, 0.0))),
    )
    records = jnp.where(first_real, records, 0.0)

    for m in range(2):
        pack[m] = records[:, m * LANES : (m + 1) * LANES]

    @pl.when(r == 0)
    def _():
        pack_in[2] = jnp.zeros((8, LANES), F32)

    east_out = remote(pack.at[0], pack_in.at[0], 5, 3, r, east)
    west_out = remote(pack.at[0], pack_in.at[1], 6, 4, r, west)
    north_out = remote(pack.at[1], pack_in.at[2], 7, 5, r + 1, p)
    over_out = remote(pack.at[1], pack_in.at[3], 7, 6, r, across)
    south_out = remote(pack.at[1], pack_in.at[3], 8, 6, r - 1, p)

    @pl.when(top)
    def _():
        over_out.start()

    @pl.when(r < n_lat - 1)
    def _():
        north_out.start()

    @pl.when(r > 0)
    def _():
        south_out.start()

    east_out.start()
    west_out.start()

    @pl.when(later)
    def _():
        gather_rest()

    corners = halo_corners(
        wide, i_row, j_row, k_row, together(gathered, wide), top, sides, nrow_in, cnr_in
    )
    moved = advanced(corners, position)
    code = (1 + i_row + cols * (j_row + rows * k_row)).astype(F32)
    kept = placed(jnp.where(sub < 3, moved, jnp.where(sub == 3, code, 0.0)), stay_ref[...])

    east_out.wait_recv()
    west_out.wait_recv()

    @pl.when(r > 0)
    def _():
        north_out.wait_recv()

    over_out.wait_recv()

    from_north = jnp.where(top, pltpu.roll(pack_in[3], half, 1), pack_in[3])
    arrivals = jnp.concatenate(
        [
            jnp.where(lane < half, pack_in[0], pack_in[1]),
            jnp.where(lane < half, pack_in[2], from_north),
        ],
        axis=1,
    )
    present = jnp.where(arrivals > 0.5, 1.0, 0.0)
    order, filled = ranked(present, jnp.broadcast_to(total[0:1], (8, LANES)))
    arrive_to = jnp.where(present[3:4] > 0.5, order[3:4], -1.0).astype(I32)
    joined = placed(arrivals, slots_of(arrive_to, slots))
    result = joined + jnp.concatenate([kept, jnp.zeros((8, slots - wide), F32)], axis=1)
    out_ref[...] = jnp.where(iota((8, slots), 0) == 4, filled[3:4, 0:1], result)

    col_out.wait_send()
    east_out.wait_send()
    west_out.wait_send()
    north_out.wait_send()

    @pl.when(r > 0)
    def _():
        row_out.wait_send()
        cnr_out.wait_send()
        south_out.wait_send()

    @pl.when(top)
    def _():
        fold_out.wait_send()

    @pl.when(away)
    def _():
        cfold_out.wait_send()


def decode(rows, cols, result_ref, new_off, new_cell, new_count):
    for n in range(3):
        new_off[n] = result_ref[n : n + 1, :]
    code = jnp.maximum(result_ref[3:4, :].astype(I32) - 1, 0)
    new_cell[0] = code & (cols - 1)
    new_cell[1] = (code // cols) & (rows - 1)
    new_cell[2] = code // (cols * rows)
    new_count[...] = result_ref[4:5, 0:1].astype(I32)


def shards(velocity, offsets, cells, counts, moves):
    _, depth, rows, cols = velocity.shape
    slots = offsets.shape[2]
    live = slots * 3 // 4
    wide = pl.cdiv(live, LANES) * LANES
    deep = pl.cdiv(depth, 16) * 16
    dims = (depth, rows, cols, slots, live, lax.axis_size("lat"), lax.axis_size("lon"))
    groups = pl.cdiv(depth * rows, 8 * LANES) * 8
    listed = pl.cdiv(2 * wide // LANES, 8) * 8
    vmem = pl.BlockSpec(memory_space=pltpu.VMEM)
    hbm = pl.BlockSpec(memory_space=pltpu.HBM)
    velocity, offsets, cells, moves = (
        pltpu.with_memory_space_constraint(x, pltpu.HBM) for x in (velocity, offsets, cells, moves)
    )
    result = pl.pallas_call(
        functools.partial(kernel, dims),
        out_shape=jax.ShapeDtypeStruct((8, slots), F32),
        in_specs=[hbm] * 5,
        out_specs=vmem,
        scratch_shapes=[
            pltpu.VMEM((3, depth, rows, cols), BF16),
            pltpu.VMEM((3, 1, slots), F32),
            pltpu.VMEM((3, 1, slots), I32),
            pltpu.VMEM((1, slots), I32),
            pltpu.VMEM((1, 1), I32),
            pltpu.VMEM((2 * deep * rows * 4 + 8 * rows * 4, LANES), F32),
            pltpu.VMEM((listed, LANES), I32),
            pltpu.SMEM((listed, LANES), I32),
            pltpu.VMEM((8, LANES), I32),
            pltpu.SMEM((8, LANES), I32),
            pltpu.VMEM((4, wide // LANES, 8, LANES), F32),
            pltpu.VMEM((4, 2, 8, LANES), F32),
            pltpu.VMEM((wide, wide), BF16),
            pltpu.VMEM((6, groups, LANES), F32),
            pltpu.VMEM((3, groups, LANES), BF16),
            pltpu.VMEM((2 * deep + 16, 3 * LANES), BF16),
            pltpu.VMEM((2 * deep + 16, 3 * LANES), BF16),
            pltpu.VMEM((8, LANES), F32),
            pltpu.VMEM((8, LANES), F32),
            pltpu.VMEM((3, groups, LANES), BF16),
            pltpu.VMEM((2 * deep + 16, 3 * LANES), BF16),
            pltpu.VMEM((8, LANES), F32),
            pltpu.VMEM((2, 8, LANES), F32),
            pltpu.VMEM((4, 8, LANES), F32),
            pltpu.SemaphoreType.DMA((rows // 8,)),
            pltpu.SemaphoreType.DMA((4,)),
            pltpu.SemaphoreType.DMA((9,)),
            pltpu.SemaphoreType.DMA((7,)),
            pltpu.SemaphoreType.DMA,
            pltpu.SemaphoreType.DMA((2,)),
        ],
        compiler_params=pltpu.CompilerParams(
            collective_id=0, has_side_effects=True, vmem_limit_bytes=32 * 1024 * 1024
        ),
        name="advance",
    )(velocity, offsets, cells, counts, moves)
    return pl.pallas_call(
        functools.partial(decode, rows, cols),
        out_shape=(
            jax.ShapeDtypeStruct((3, 1, slots), F32),
            jax.ShapeDtypeStruct((3, 1, slots), I32),
            jax.ShapeDtypeStruct((1, 1), I32),
        ),
        in_specs=[vmem],
        out_specs=(vmem, vmem, vmem),
        compiler_params=pltpu.CompilerParams(vmem_limit_bytes=1024 * 1024),
        name="decode",
    )(result)


def solution(mesh):
    placed_in = (
        P(None, None, "lat", "lon"),
        P(None, "lat", "lon"),
        P(None, "lat", "lon"),
        P("lat", "lon"),
        P("lat", "lon"),
    )
    return jax.shard_map(
        shards,
        mesh=mesh,
        in_specs=placed_in,
        out_specs=(P(None, "lat", "lon"), P(None, "lat", "lon"), P("lat", "lon")),
        check_vma=False,
    )
```

```python
import functools

import jax
import jax.numpy as jnp
from jax import lax
from jax.experimental import pallas as pl
from jax.experimental.pallas import tpu as pltpu
from jax.sharding import PartitionSpec as P

MESH = pl.DeviceIdType.MESH
CAP = 48
LANES = 128
F32, BF16, I32 = jnp.float32, jnp.bfloat16, jnp.int32
NT = (((1,), (1,)), ((), ()))
TN = (((0,), (0,)), ((), ()))


def iota(shape, dim):
    return lax.broadcasted_iota(I32, shape, dim)


def thirds(x):
    high = x.astype(BF16)
    rest = x - high.astype(F32)
    mid = rest.astype(BF16)
    low = (rest - mid.astype(F32)).astype(BF16)
    return jnp.concatenate([high.astype(F32), mid.astype(F32), low.astype(F32)], axis=0).astype(BF16)


def slots_of(target, size):
    return jnp.where(iota((size, target.shape[1]), 0) == target, 1.0, 0.0).astype(BF16)


def placed(records, onehot):
    out = lax.dot_general(thirds(records), onehot, NT, preferred_element_type=F32)
    return out[0:8] + out[8:16] + out[16:24]


def velocity_at(corners, a_row, b_row, c_row):
    sub = iota((8, a_row.shape[1]), 0)
    wb = jnp.where(sub < 4, 1.0 - b_row, b_row)
    w0 = (wb * (1.0 - c_row)).astype(BF16).astype(F32)
    w1 = (wb * c_row).astype(BF16).astype(F32)
    sums = []
    for d in range(2):
        s = w0 * corners[0][d] + w1 * corners[1][d]
        sums.append(s + pltpu.roll(s, 4, 0))
    return (1.0 - a_row) * sums[0] + a_row * sums[1]


def lookups(w, i_row, j_row, k_row, top, deep, groups, rows):
    cols, per = 2 * LANES, LANES // rows

    def twice(x):
        return jnp.concatenate([x] * 2, axis=1)

    def hot(size, at):
        return jnp.where(iota((size, 2 * w), 0) == at, 1.0, 0.0).astype(BF16)

    k2 = jnp.concatenate([k_row, k_row + 1], axis=1)
    j2 = twice(j_row)
    outer = twice(jnp.where(i_row == cols - 1, groups, 0))
    at_side = hot(8 * groups, (k2 & (per - 1)) * (2 * groups) + outer + lax.shift_right_logical(k2, per.bit_length() - 1))
    base = twice(jnp.where(top, cols - 1 - i_row, i_row))
    second = base >= LANES
    inner = base & (LANES - 1)
    at_row = hot(2 * deep, k2 + jnp.where(second, deep, 0))
    at_level = hot(LANES, k2)
    return at_side, at_row, at_level, j2, second, inner


def halo_corners(w, i_row, j_row, plan, inside, top, sides, nrow_in, cnr_in):
    at_side, at_row, at_level, j2, second, inner = plan
    rows = sides[0].shape[0]
    deep = (nrow_in.shape[0] - 16) // 2
    sub2 = iota((8, 2 * w), 0)

    eastern = jnp.zeros((8, 2 * w), F32)
    hits = [iota((rows, 2 * w), 0) == j2 + dj for dj in range(2)]
    for c in range(3):
        found = jnp.dot(sides[c], at_side, preferred_element_type=F32)
        for dj in range(2):
            value = jnp.sum(jnp.where(hits[dj], found, 0.0), axis=0, keepdims=True)
            eastern = jnp.where(sub2 == 4 * dj + c, value, eastern)

    few = jnp.concatenate([cnr_in[...], nrow_in[2 * deep :, 0:LANES].astype(F32)], axis=0).astype(BF16)
    ends = jnp.dot(few, at_level, preferred_element_type=F32)
    last = pltpu.roll(jnp.where(second, ends[0:8], ends[8:16]), 4, 0)

    pair = [jnp.zeros((8, 2 * w), F32), last]
    lane_id = iota((LANES, 2 * w), 0)
    hits = [lane_id == inner, lane_id == inner + 1]
    for c in range(3):
        found = lax.dot_general(
            nrow_in[0 : 2 * deep, c * LANES : (c + 1) * LANES], at_row, TN, preferred_element_type=F32
        )
        for d in range(2):
            value = jnp.sum(jnp.where(hits[d], found, 0.0), axis=0, keepdims=True)
            put = sub2 == 4 + c
            pair[d] = jnp.where(put & (inner < LANES - 1) if d else put, value, pair[d])

    sign = jnp.where(top, -1.0, 1.0)
    north = [sign * jnp.where(top, pair[1 - d], pair[d]) for d in range(2)]
    lower = iota((8, w), 0) >= 4
    corners = []
    for dk in range(2):
        part = slice(dk * w, (dk + 1) * w)
        out = []
        for d in range(2):
            here = inside[dk][d]
            if d == 1:
                here = jnp.where((i_row & (LANES - 1)) == LANES - 1, eastern[:, part], here)
            out.append(jnp.where(lower & (j_row == rows - 1), north[d][:, part], here))
        corners.append(out)
    return corners


def advanced(corners, position):
    first = velocity_at(corners, position[0:1], position[1:2], position[2:3])
    middle = position + 0.5 * first
    return position + velocity_at(corners, middle[0:1], middle[1:2], middle[2:3])


def kernel(
    dims, vel_hbm, off_hbm, cell_hbm, count_hbm, move_hbm,
    out_ref,
    vel, off_ref, cell_ref, move_ref, count_ref, table, where_ref, where_smem, first_ref, first_smem,
    gathered, first_gathered, stay_ref,
    side, column, nrow, nfold, cnr, cfold, col_in, nrow_in, cnr_in,
    pack, pack_in, vsem, isem, send, recv, lsem, asem,
):
    depth, rows, cols, slots, live, n_lat, n_lon = dims
    wide = pl.cdiv(live, LANES) * LANES
    tiles = wide // LANES
    half = LANES // 2
    few = 4 * half
    level = rows * 4
    deep = pl.cdiv(depth, 16) * 16
    span = deep * level
    per = LANES // rows
    groups = side.shape[1]
    r, p = lax.axis_index("lat"), lax.axis_index("lon")
    east, west = lax.rem(p + 1, n_lon), lax.rem(p + n_lon - 1, n_lon)
    across, corner = n_lon - 1 - p, lax.rem(n_lon - p, n_lon)
    top = r == n_lat - 1
    away = jnp.logical_and(top, corner != p)

    smalls = [(cell_hbm, cell_ref), (move_hbm, move_ref), (count_hbm, count_ref), (off_hbm, off_ref)]
    smalls = [pltpu.make_async_copy(src, dst, isem.at[n]) for n, (src, dst) in enumerate(smalls)]
    bands = [slice(8 * n, 8 * n + 8) for n in range(rows // 8)]
    bands = [bands[0], bands[-1]] + bands[1:-1]
    loads = [
        pltpu.make_async_copy(vel_hbm.at[:, :, band, :], vel.at[:, :, band, :], vsem.at[n])
        for n, band in enumerate(bands)
    ]
    loads[0].start()
    for copy in smalls + loads[1:]:
        copy.start()

    barrier = pltpu.get_barrier_semaphore()

    def greet(lat, lon):
        pl.semaphore_signal(barrier, inc=1, device_id=(lon, lat), device_id_type=MESH)

    greet(r, east)
    greet(r, west)

    @pl.when(r < n_lat - 1)
    def _():
        greet(r + 1, p)
        greet(r + 1, east)

    @pl.when(r > 0)
    def _():
        greet(r - 1, p)

    @pl.when(top)
    def _():
        greet(r, across)

    @pl.when(away)
    def _():
        greet(r, corner)

    lane = iota((8, LANES), 1)
    sub = iota((8, wide), 0)
    for part in range(2):
        table[pl.ds(part * span + depth * level, span - depth * level), :] = jnp.zeros(
            (span - depth * level, LANES), F32
        )
    side[...] = jnp.zeros_like(side)
    gathered[...] = jnp.zeros_like(gathered)
    first_gathered[...] = jnp.zeros_like(first_gathered)
    first_lane = jnp.where(lane == 0, 1.0, 0.0).astype(BF16)

    def build(n):
        band = bands[n]
        loads[n].wait()

        def body(step, carry):
            for u in range(5):
                k = step * 5 + u
                for c in range(3):
                    for h in range(2):
                        at = h * span + k * level + 4 * band.start + c
                        table[pl.ds(at, 8, stride=4), :] = vel[c, k, band, h * LANES : (h + 1) * LANES].astype(F32)
            return carry

        lax.fori_loop(0, depth // 5, body, 0)

    def edge(target, ends, row):
        firsts = [jnp.zeros((8, deep), F32)] * 2
        for h in range(2):
            for c in range(3):
                blocks = []
                for block in range(deep // 8):
                    at = h * span + block * 8 * level + 4 * row + c
                    blocks.append(table[pl.ds(at, 8, stride=level), :])
                plane = jnp.concatenate(blocks, axis=0).astype(BF16)
                target[pl.ds(h * deep, deep), pl.ds(c * LANES, LANES)] = plane
                pick = jnp.where((lane == 0) & (iota((8, LANES), 0) == c), 1.0, 0.0).astype(BF16)
                firsts[h] = firsts[h] + lax.dot_general(pick, plane, NT, preferred_element_type=F32)
        pad = jnp.zeros((8, LANES - deep), F32)
        tail = jnp.concatenate([jnp.concatenate([firsts[1], pad], axis=1), jnp.zeros((8, LANES), F32)], axis=0)
        target[2 * deep : 2 * deep + 16, :] = jnp.concatenate([tail, jnp.zeros((16, 2 * LANES), F32)], axis=1).astype(BF16)
        ends[...] = jnp.concatenate([firsts[0], pad], axis=1)

    def remote(src, dst, s, t, lat, lon):
        return pltpu.make_async_remote_copy(
            src, dst, send.at[s], recv.at[t], device_id=(lon, lat), device_id_type=MESH
        )

    col_out = remote(column, col_in, 0, 0, r, west)
    row_out = remote(nrow, nrow_in, 1, 1, r - 1, p)
    cnr_out = remote(cnr, cnr_in, 2, 2, r - 1, west)
    fold_out = remote(nfold, nrow_in, 3, 1, r, across)
    cfold_out = remote(cfold, cnr_in, 4, 2, r, corner)
    cfold_here = pltpu.make_async_copy(cfold, cnr_in, lsem)

    build(0)
    edge(nrow, cnr, 0)
    peers = 2 + 2 * (r > 0).astype(I32) + (r < n_lat - 1).astype(I32) + top.astype(I32) + away.astype(I32)

    def send_rows(*first):
        pl.semaphore_wait(barrier, peers)
        for copy in first:
            copy.start()

        @pl.when(r > 0)
        def _():
            cnr_out.start()
            row_out.start()

    def send_fold():
        @pl.when(top)
        def _():
            fold_out.start()

        @pl.when(away)
        def _():
            cfold_out.start()

    patient = p == 0
    eager = jnp.logical_not(patient)

    @pl.when(eager)
    def _():
        send_rows()

    for small in smalls:
        small.wait()

    i_row, j_row, k_row = (cell_ref[n, :, 0:wide] for n in range(3))
    motion = move_ref[:, 0:wide]
    valid = iota((1, wide), 1) < count_ref[...]
    chosen = jnp.where((sub == motion) & valid, 1.0, 0.0)
    before = jnp.where(iota((LANES, LANES), 0) < iota((LANES, LANES), 1), 1.0, 0.0).astype(BF16)
    upto = jnp.concatenate([before, jnp.ones((LANES, LANES), BF16)], axis=1)

    def ranked(flags, total):
        out = []
        for t in range(flags.shape[1] // LANES):
            sums = jnp.dot(
                flags[:, t * LANES : (t + 1) * LANES].astype(BF16), upto, preferred_element_type=F32
            )
            out.append(sums[:, :LANES] + total)
            total = total + sums[:, LANES:]
        return jnp.concatenate(out, axis=1), total

    rank, total = ranked(chosen, jnp.zeros((8, LANES), F32))
    stay_to = jnp.where(chosen[0:1] > 0.5, rank[0:1], -1.0).astype(I32)
    slot_to = rank + (half * (sub - 1)).astype(F32)
    leaving = (sub >= 1) & (chosen > 0.5)
    leave_to = (jnp.sum(jnp.where(leaving, slot_to + 1.0, 0.0), axis=0, keepdims=True) - 1.0).astype(I32)
    position = jnp.zeros((8, wide), F32)
    for n in range(3):
        position = jnp.where(sub == n, off_ref[n, :, 0:wide], position)
    marks = jnp.where(sub == 0, i_row, jnp.where(sub == 1, j_row, jnp.where(sub == 2, k_row, 1)))
    raw = lax.dot_general(
        jnp.concatenate([thirds(position).astype(F32), marks.astype(F32)], axis=0).astype(BF16),
        slots_of(leave_to, few), NT, preferred_element_type=F32,
    )
    first_position = raw[0:8] + raw[8:16] + raw[16:24]
    first_i, first_j, first_k = (
        jnp.clip(raw[24 + n : 25 + n].astype(I32), 0, top_value)
        for n, top_value in enumerate((cols - 1, rows - 1, depth - 2))
    )
    first_real = raw[27:28] > 0.5

    def words(i, j, k, target):
        start = jnp.clip(jnp.where(i >= LANES, span, 0) + k * level + 4 * j, 0, 2 * span - level - 8)
        start = start * LANES + ((iota(i.shape, 1) - i) & (LANES - 1))
        for t in range(i.shape[1] // LANES):
            part = start[:, t * LANES : (t + 1) * LANES]
            target[2 * t : 2 * t + 1, :] = part
            target[2 * t + 1 : 2 * t + 2, :] = pltpu.roll(part, half, 1)

    first_ref[...] = jnp.zeros_like(first_ref)
    where_ref[...] = jnp.zeros_like(where_ref)
    words(first_i, first_j, first_k, first_ref)
    words(i_row, j_row, k_row, where_ref)
    addresses = [
        pltpu.make_async_copy(first_ref, first_smem, asem.at[0]),
        pltpu.make_async_copy(where_ref, where_smem, asem.at[1]),
    ]
    for copy in addresses:
        copy.start()
    stay_ref[...] = slots_of(stay_to, wide)

    build(1)

    @pl.when(top)
    def _():
        edge(nfold, cfold, rows - 1)

    @pl.when(eager)
    def _():
        send_fold()

    @pl.when(jnp.logical_and(top, corner == p))
    def _():
        cfold_here.start()

    for n in range(2, len(bands)):
        build(n)

    for c in range(3):
        for h in range(2):
            plane = vel[c, :, :, h * LANES : (h + 1) * LANES].reshape(depth * rows, LANES)
            line = lax.dot_general(first_lane, plane, NT, preferred_element_type=F32)[0:1]
            for g in range(pl.cdiv(depth, per)):
                n = min(LANES, depth * rows - g * LANES)
                side[h * 3 + c, g : g + 1, 0:n] = line[:, g * LANES : g * LANES + n]
    column[...] = side[0:3].astype(BF16)
    @pl.when(eager)
    def _():
        col_out.start()

    def gather(source, target, count):
        def body(step, carry):
            base = (step & 1) * half
            group = step >> 1
            ahead = lane - base
            accs = [target[n, group] for n in range(4)]
            for u in range(count):
                word = source[step, u]
                at, shift = word >> 7, word & (LANES - 1)
                here = ahead == u
                there = ahead == u + 1 if u < half - 1 else lane == ((base + half) & (LANES - 1))
                for dk in range(2):
                    turned = pltpu.roll(table[pl.ds(at + dk * level, 8), :], shift, 1)
                    accs[2 * dk] = jnp.where(here, turned, accs[2 * dk])
                    accs[2 * dk + 1] = jnp.where(there, turned, accs[2 * dk + 1])
            for n in range(4):
                target[n, group] = accs[n]
            return carry

        return body

    def together(source, w):
        out = []
        for dk in range(2):
            low = [source[2 * dk, t] for t in range(w // LANES)]
            high = [pltpu.roll(source[2 * dk + 1, t], LANES - 1, 1) for t in range(w // LANES)]
            out.append([jnp.concatenate(low, axis=1), jnp.concatenate(high, axis=1)])
        return out

    for copy in addresses:
        copy.wait()
    lax.fori_loop(0, 4, gather(first_smem, first_gathered, CAP), 0)

    later = (r % 2 == 0) & (p > 0)

    def gather_rest():
        lax.fori_loop(0, live // half, gather(where_smem, gathered, half), 0)

    @pl.when(jnp.logical_not(later))
    def _():
        gather_rest()

    @pl.when(patient)
    def _():
        send_rows(col_out)
        send_fold()


    go = iota((1, few), 1) // half + 1
    folding = (go == 3) & top
    last_i, last_j = cols - 1, rows - 1
    new_i = jnp.where(
        go == 1, 0, jnp.where(go == 2, last_i, jnp.where(folding, last_i - first_i, first_i))
    )
    new_j = jnp.where(
        go == 3, jnp.where(top, last_j, 0), jnp.where(go == 4, last_j, first_j)
    )
    code = jnp.where(first_real, 1 + new_i + cols * (new_j + rows * first_k), 0).astype(F32)

    first_plan = lookups(few, first_i, first_j, first_k, top, deep, groups, rows)
    cnr_wait = remote(cnr, cnr_in, 2, 2, r, west)
    col_out.wait_recv()
    row_out.wait_recv()

    @pl.when(jnp.logical_or(jnp.logical_not(top), corner != p))
    def _():
        cnr_wait.wait_recv()

    @pl.when(jnp.logical_and(top, corner == p))
    def _():
        cfold_here.wait()

    sides = []
    for c in range(3):
        lines = jnp.concatenate([side[3 + c], col_in[c].astype(F32)], axis=0)
        lines = [lines if m == 0 else pltpu.roll(lines, LANES - m * rows, 1) for m in range(per)]
        sides.append(jnp.concatenate(lines, axis=0).T[0:rows].astype(BF16))

    corners = halo_corners(
        few, first_i, first_j, first_plan, together(first_gathered, few), top, sides, nrow_in, cnr_in
    )
    moved = advanced(corners, first_position)
    na, nb, nc = moved[0:1], moved[1:2], moved[2:3]
    new_a = jnp.where(go == 1, na - 1.0, jnp.where(go == 2, na + 1.0, jnp.where(folding, 1.0 - na, na)))
    new_b = jnp.where(go == 3, jnp.where(top, 2.0 - nb, nb - 1.0), jnp.where(go == 4, nb + 1.0, nb))
    sub_few = iota((8, few), 0)
    records = jnp.where(
        sub_few == 0, new_a,
        jnp.where(sub_few == 1, new_b, jnp.where(sub_few == 2, nc, jnp.where(sub_few == 3, code, 0.0))),
    )
    records = jnp.where(first_real, records, 0.0)

    for m in range(2):
        pack[m] = records[:, m * LANES : (m + 1) * LANES]

    @pl.when(r == 0)
    def _():
        pack_in[2] = jnp.zeros((8, LANES), F32)

    east_out = remote(pack.at[0], pack_in.at[0], 5, 3, r, east)
    west_out = remote(pack.at[0], pack_in.at[1], 6, 4, r, west)
    north_out = remote(pack.at[1], pack_in.at[2], 7, 5, r + 1, p)
    over_out = remote(pack.at[1], pack_in.at[3], 7, 6, r, across)
    south_out = remote(pack.at[1], pack_in.at[3], 8, 6, r - 1, p)

    @pl.when(top)
    def _():
        over_out.start()

    @pl.when(r < n_lat - 1)
    def _():
        north_out.start()

    @pl.when(r > 0)
    def _():
        south_out.start()

    east_out.start()
    west_out.start()

    @pl.when(later)
    def _():
        gather_rest()

    corners = halo_corners(
        wide, i_row, j_row, lookups(wide, i_row, j_row, k_row, top, deep, groups, rows), together(gathered, wide), top, sides, nrow_in, cnr_in
    )
    moved = advanced(corners, position)
    code = (1 + i_row + cols * (j_row + rows * k_row)).astype(F32)
    kept = placed(jnp.where(sub < 3, moved, jnp.where(sub == 3, code, 0.0)), stay_ref[...])

    east_out.wait_recv()
    west_out.wait_recv()

    @pl.when(r > 0)
    def _():
        north_out.wait_recv()

    over_out.wait_recv()

    from_north = jnp.where(top, pltpu.roll(pack_in[3], half, 1), pack_in[3])
    arrivals = jnp.concatenate(
        [
            jnp.where(lane < half, pack_in[0], pack_in[1]),
            jnp.where(lane < half, pack_in[2], from_north),
        ],
        axis=1,
    )
    present = jnp.where(arrivals > 0.5, 1.0, 0.0)
    order, filled = ranked(present, jnp.broadcast_to(total[0:1], (8, LANES)))
    arrive_to = jnp.where(present[3:4] > 0.5, order[3:4], -1.0).astype(I32)
    joined = placed(arrivals, slots_of(arrive_to, slots))
    result = joined + jnp.concatenate([kept, jnp.zeros((8, slots - wide), F32)], axis=1)
    out_ref[...] = jnp.where(iota((8, slots), 0) == 4, filled[3:4, 0:1], result)

    col_out.wait_send()
    east_out.wait_send()
    west_out.wait_send()
    north_out.wait_send()

    @pl.when(r > 0)
    def _():
        row_out.wait_send()
        cnr_out.wait_send()
        south_out.wait_send()

    @pl.when(top)
    def _():
        fold_out.wait_send()

    @pl.when(away)
    def _():
        cfold_out.wait_send()


def decode(rows, cols, result_ref, new_off, new_cell, new_count):
    for n in range(3):
        new_off[n] = result_ref[n : n + 1, :]
    code = jnp.maximum(result_ref[3:4, :].astype(I32) - 1, 0)
    new_cell[0] = code & (cols - 1)
    new_cell[1] = (code // cols) & (rows - 1)
    new_cell[2] = code // (cols * rows)
    new_count[...] = result_ref[4:5, 0:1].astype(I32)


def shards(velocity, offsets, cells, counts, moves):
    _, depth, rows, cols = velocity.shape
    slots = offsets.shape[2]
    live = slots * 3 // 4
    wide = pl.cdiv(live, LANES) * LANES
    deep = pl.cdiv(depth, 16) * 16
    dims = (depth, rows, cols, slots, live, lax.axis_size("lat"), lax.axis_size("lon"))
    groups = pl.cdiv(depth * rows, 8 * LANES) * 8
    listed = pl.cdiv(2 * wide // LANES, 8) * 8
    vmem = pl.BlockSpec(memory_space=pltpu.VMEM)
    hbm = pl.BlockSpec(memory_space=pltpu.HBM)
    velocity, offsets, cells, moves = (
        pltpu.with_memory_space_constraint(x, pltpu.HBM) for x in (velocity, offsets, cells, moves)
    )
    result = pl.pallas_call(
        functools.partial(kernel, dims),
        out_shape=jax.ShapeDtypeStruct((8, slots), F32),
        in_specs=[hbm] * 5,
        out_specs=vmem,
        scratch_shapes=[
            pltpu.VMEM((3, depth, rows, cols), BF16),
            pltpu.VMEM((3, 1, slots), F32),
            pltpu.VMEM((3, 1, slots), I32),
            pltpu.VMEM((1, slots), I32),
            pltpu.VMEM((1, 1), I32),
            pltpu.VMEM((2 * deep * rows * 4 + 8 * rows * 4, LANES), F32),
            pltpu.VMEM((listed, LANES), I32),
            pltpu.SMEM((listed, LANES), I32),
            pltpu.VMEM((8, LANES), I32),
            pltpu.SMEM((8, LANES), I32),
            pltpu.VMEM((4, wide // LANES, 8, LANES), F32),
            pltpu.VMEM((4, 2, 8, LANES), F32),
            pltpu.VMEM((wide, wide), BF16),
            pltpu.VMEM((6, groups, LANES), F32),
            pltpu.VMEM((3, groups, LANES), BF16),
            pltpu.VMEM((2 * deep + 16, 3 * LANES), BF16),
            pltpu.VMEM((2 * deep + 16, 3 * LANES), BF16),
            pltpu.VMEM((8, LANES), F32),
            pltpu.VMEM((8, LANES), F32),
            pltpu.VMEM((3, groups, LANES), BF16),
            pltpu.VMEM((2 * deep + 16, 3 * LANES), BF16),
            pltpu.VMEM((8, LANES), F32),
            pltpu.VMEM((2, 8, LANES), F32),
            pltpu.VMEM((4, 8, LANES), F32),
            pltpu.SemaphoreType.DMA((rows // 8,)),
            pltpu.SemaphoreType.DMA((4,)),
            pltpu.SemaphoreType.DMA((9,)),
            pltpu.SemaphoreType.DMA((7,)),
            pltpu.SemaphoreType.DMA,
            pltpu.SemaphoreType.DMA((2,)),
        ],
        compiler_params=pltpu.CompilerParams(
            collective_id=0, has_side_effects=True, vmem_limit_bytes=32 * 1024 * 1024
        ),
        name="advance",
    )(velocity, offsets, cells, counts, moves)
    return pl.pallas_call(
        functools.partial(decode, rows, cols),
        out_shape=(
            jax.ShapeDtypeStruct((3, 1, slots), F32),
            jax.ShapeDtypeStruct((3, 1, slots), I32),
            jax.ShapeDtypeStruct((1, 1), I32),
        ),
        in_specs=[vmem],
        out_specs=(vmem, vmem, vmem),
        compiler_params=pltpu.CompilerParams(vmem_limit_bytes=1024 * 1024),
        name="decode",
    )(result)


def solution(mesh):
    placed_in = (
        P(None, None, "lat", "lon"),
        P(None, "lat", "lon"),
        P(None, "lat", "lon"),
        P("lat", "lon"),
        P("lat", "lon"),
    )
    return jax.shard_map(
        shards,
        mesh=mesh,
        in_specs=placed_in,
        out_specs=(P(None, "lat", "lon"), P(None, "lat", "lon"), P("lat", "lon")),
        check_vma=False,
    )
```
